32 devices in a mesh: rep: 2 (over z, core), dp: 16 (over x, y).
Axes of the slice: x: 4, y: 4, z: 1, core: 2. Of those that a mesh axis runs over, the one named last changes fastest.
The devices are a block of a 4x4x8 slice.
Arguments:
- x: bfloat16 [32, 1024, 512], P(('rep', 'dp')), parts along dimension 0
- dy: bfloat16 [32, 1024, 512], P(('rep', 'dp')), parts along dimension 0
- w_gate: bfloat16 [2, 512, 8192], replicated
- w_up: bfloat16 [2, 512, 8192], replicated
- w_down: bfloat16 [2, 8192, 512], replicated
- m_w_gate: float32 [2, 512, 8192], P(None, 'dp')
- m_w_up: float32 [2, 512, 8192], P(None, 'dp')
- m_w_down: float32 [2, 8192, 512], P(None, 'dp')
- v_w_gate: float32 [2, 512, 8192], P(None, 'dp')
- v_w_up: float32 [2, 512, 8192], P(None, 'dp')
- v_w_down: float32 [2, 8192, 512], P(None, 'dp')
Outputs:
- output 1: bfloat16 [4, 512, 8192], P('rep'), parts along dimension 0
- output 2: bfloat16 [4, 512, 8192], P('rep'), parts along dimension 0
- output 3: bfloat16 [4, 8192, 512], P('rep'), parts along dimension 0
- output 4: float32 [4, 512, 8192], P('rep', 'dp'), parts along dimension 0
- output 5: float32 [4, 512, 8192], P('rep', 'dp'), parts along dimension 0
- output 6: float32 [4, 8192, 512], P('rep', 'dp'), parts along dimension 0
- output 7: float32 [4, 512, 8192], P('rep', 'dp'), parts along dimension 0
- output 8: float32 [4, 512, 8192], P('rep', 'dp'), parts along dimension 0
- output 9: float32 [4, 8192, 512], P('rep', 'dp'), parts along dimension 0
There are 2 independent parts. The reference program is written for one: setup_inputs(seed, part) draws one part's arguments, and reference() takes and returns one part's arrays. A program takes and returns all parts, laid end to end along the dimension named above; an argument that names none is the same for every part.
All inputs are finite; a program needn't handle non-finite values.
Results may differ from the reference program's by a relative error of at most 0.022.
Values are sent between devices in bfloat16 or wider.
A program may use at most 768 MiB of HBM per device.

```python
import jax
import jax.numpy as jnp
from jax import lax

SEQUENCES = 16
TOKENS = 1024
D = 512
FF = 8192
LAYERS = 2
NAMES = ("w_gate", "w_up", "w_down")
SHAPES = {"w_gate": (LAYERS, D, FF), "w_up": (LAYERS, D, FF), "w_down": (LAYERS, FF, D)}


def bump(key, n, height):
    away = (jnp.arange(n, dtype=jnp.int32) - jax.random.randint(key, (), 0, n, jnp.int32)) % n
    return jnp.where(away < n // 8, height, 1.0)


def together(key, own, strength):
    shared = jax.random.normal(key, own.shape[1:], jnp.float32)
    return (own + strength * shared) * lax.rsqrt(1 + strength * strength)


def setup_inputs(seed: int = 0, part: int = 0) -> dict:
    kx, kdy, ka, kb, kz, kf, kh, kl, *keys = jax.random.split(jax.random.key(seed), 8 + 3 * len(NAMES))
    kx, kdy, ka, kb = (jax.random.fold_in(k, part) for k in (kx, kdy, ka, kb))
    kw, km, kv = (keys[i::3] for i in range(3))
    shape = (SEQUENCES, TOKENS, D)
    much_x, much_dy = jax.random.uniform(kz, (2,), jnp.float32, 0.0, 1.0)
    loud = 2.0 ** jax.random.uniform(jax.random.fold_in(kz, 1), (), jnp.float32, -1.0, 2.0)
    layers = 2.0 ** jax.random.uniform(kl, (LAYERS, 1, 1), jnp.float32, -1.0, 1.0)
    x = together(ka, jax.random.normal(kx, shape, jnp.float32), much_x) * bump(kf, D, 4.0)
    dy = together(kb, jax.random.normal(kdy, shape, jnp.float32), much_dy)
    drawn = {"x": x.astype(jnp.bfloat16), "dy": (loud * dy * (SEQUENCES * TOKENS) ** -0.5).astype(jnp.bfloat16)}
    for key, name in zip(kw, NAMES, strict=True):
        w = jax.random.normal(key, SHAPES[name], jnp.float32) * SHAPES[name][1] ** -0.5
        drawn[name] = (w * {"w_gate": 1.0, "w_up": bump(kh, FF, 4.0), "w_down": layers}[name]).astype(jnp.bfloat16)
    for key, name in zip(km, NAMES, strict=True):
        drawn[f"m_{name}"] = 0.1 * jax.random.normal(key, SHAPES[name], jnp.float32)
    for key, name in zip(kv, NAMES, strict=True):
        drawn[f"v_{name}"] = jax.random.uniform(key, SHAPES[name], jnp.float32, 0.005, 0.015)
    return drawn


def matmul(a, w):
    return jnp.dot(a, w, preferred_element_type=jnp.float32).astype(jnp.bfloat16)


def normed(h):
    wide = h.astype(jnp.float32)
    scale = lax.rsqrt(jnp.mean(wide**2, -1, keepdims=True) + 1e-6)
    return (wide * scale).astype(jnp.bfloat16)


def layer(h, w):
    a = normed(h)
    gate = jnp.dot(a, w["w_gate"], preferred_element_type=jnp.float32)
    up = jnp.dot(a, w["w_up"], preferred_element_type=jnp.float32)
    return h + matmul((jax.nn.silu(gate) * up).astype(jnp.bfloat16), w["w_down"])


def adamw(w, m, v, g):
    m = 0.9 * m + 0.1 * g
    v = 0.95 * v + 0.05 * g * g
    step = m * lax.rsqrt(v + 1e-8) + 0.1 * w
    return (w - 0.02 * step).astype(jnp.bfloat16), m, v


def clipped(gradients, sum_of_squares, count):
    factor = jnp.minimum(1.0, 0.5 * lax.rsqrt(sum_of_squares / count + 1e-30))
    return [g * factor for g in gradients]


def stack(weights, h):
    return lax.scan(lambda h, w: (layer(h, w), None), h, weights)[0]


def reference(x, dy, w_gate, w_up, w_down, m_w_gate, m_w_up, m_w_down, v_w_gate, v_w_up, v_w_down):
    weights = dict(zip(NAMES, (w_gate, w_up, w_down), strict=True))

    def take(so_far, sequence):
        h, by_y = sequence
        _, back = jax.vjp(lambda w: stack(w, h), weights)
        return jax.tree.map(lambda total, term: total + term.astype(jnp.float32), so_far, back(by_y)[0]), None

    none_yet = {name: jnp.zeros(w.shape, jnp.float32) for name, w in weights.items()}
    by_weights, _ = lax.scan(take, none_yet, (x, dy))
    gradients = [by_weights[name].astype(jnp.bfloat16).astype(jnp.float32) for name in NAMES]
    gradients = clipped(gradients, sum(jnp.sum(g * g) for g in gradients), sum(g.size for g in gradients))
    new = [
        adamw(w.astype(jnp.float32), m, v, g)
        for w, m, v, g in zip((w_gate, w_up, w_down), (m_w_gate, m_w_up, m_w_down), (v_w_gate, v_w_up, v_w_down), gradients, strict=True)
    ]
    return tuple(one[which] for which in range(3) for one in new)
```

```python
import functools
import math

import jax
import jax.numpy as jnp
from jax import lax
from jax.experimental import pallas as pl
from jax.experimental.pallas import tpu as pltpu
from jax.sharding import Mesh
from jax.sharding import PartitionSpec as P

F32, BF = jnp.float32, jnp.bfloat16
MESH = pl.DeviceIdType.MESH
MIB = 2**20
ANY = pl.BlockSpec(memory_space=pl.ANY)
DMA = pltpu.SemaphoreType.DMA
SIDE = 4


def dot(a, b):
    return jnp.dot(a, b, preferred_element_type=F32)


def dot_t(a, b):
    return lax.dot_general(a, b, (((1,), (1,)), ((), ())), preferred_element_type=F32)


def normed(h):
    wide = h.astype(F32)
    scale = lax.rsqrt(jnp.mean(wide * wide, -1, keepdims=True) + 1e-6)
    return (wide * scale).astype(BF)


def sigmoid(z):
    return 0.5 * jnp.tanh(0.5 * z) + 0.5


def ring(axis):
    me = lax.axis_index(axis)
    return me, lax.rem(me + 1, SIDE), lax.rem(me + SIDE - 1, SIDE)


def greet(peers):
    barrier = pltpu.get_barrier_semaphore()
    for axis, index in peers:
        pl.semaphore_signal(barrier, inc=1, device_id={axis: index}, device_id_type=MESH)
    pl.semaphore_wait(barrier, len(peers))


def remote(src, dst, send, recv, axis, index):
    return pltpu.make_async_remote_copy(
        src_ref=src, dst_ref=dst, send_sem=send, recv_sem=recv, device_id={axis: index}, device_id_type=MESH
    )


class Gather:
    def __init__(self, own, slots, send, recv):
        _, after, before = ring("x")
        half = own.shape[0] // 2
        top, bottom = pl.ds(0, half), pl.ds(half, half)
        c = lambda k, src, dst, to: remote(src, dst, send.at[k], recv.at[k], "x", to)
        self.first = [
            c(0, own.at[top], slots.at[0, top], after),
            c(1, own.at[bottom], slots.at[1, bottom], before),
            c(2, own.at[bottom], slots.at[0, bottom], after),
            c(3, own.at[top], slots.at[1, top], before),
        ]
        self.second = [
            c(4, slots.at[0, top], slots.at[2, top], after),
            c(5, slots.at[1, bottom], slots.at[2, bottom], before),
        ]

    def start(self):
        for copy in self.first:
            copy.start()

    def relay(self):
        for copy in self.first[:2]:
            copy.wait_recv()
        for copy in self.second:
            copy.start()

    def finish(self):
        for copy in self.first[2:] + self.second:
            copy.wait_recv()
        for copy in self.first + self.second:
            copy.wait_send()


def forward_kernel(steps, sub, x, dy, wg, wu, wd, h1, a1, a2, slots, acc, send, recv):
    j = pl.program_id(0)
    gather = Gather(dy, slots, send, recv)

    @pl.when(j == 0)
    def _():
        _, after, before = ring("x")
        greet([("x", after), ("x", before)])
        gather.start()
        a1[...] = normed(x[...])
        acc[...] = jnp.zeros_like(acc)

    @pl.when(j == steps // 2)
    def _():
        gather.relay()

    for i in range(x.shape[0] // sub):
        r = pl.ds(i * sub, sub)
        a = a1[r, :]
        gate, up = dot(a, wg[0]), dot(a, wu[0])
        acc[r, :] += dot((gate * sigmoid(gate) * up).astype(BF), wd[0])

    @pl.when(j == steps - 1)
    def _():
        h = x[...] + acc[...].astype(BF)
        h1[...] = h
        a2[...] = normed(h)
        gather.finish()


def own_kernel(steps, sub, h1, a2, dy, a2_any, a1_any, wg, wu, wd, dh1, slots, halves, accg, accu, send, recv, send1, recv1):
    j = pl.program_id(0)
    _, after, before = ring("x")
    gather = Gather(a2_any, slots, send, recv)
    half = a1_any.shape[0] // 2
    part = [
        remote(a1_any.at[pl.ds(0, half)], halves.at[0], send1.at[0], recv1.at[0], "x", after),
        remote(a1_any.at[pl.ds(half, half)], halves.at[1], send1.at[1], recv1.at[1], "x", before),
    ]

    @pl.when(j == 0)
    def _():
        greet([("x", after), ("x", before)])
        gather.start()
        accg[...] = jnp.zeros_like(accg)
        accu[...] = jnp.zeros_like(accu)

    @pl.when(j == steps // 3)
    def _():
        gather.relay()
        for copy in part:
            copy.start()

    for i in range(h1.shape[0] // sub):
        r = pl.ds(i * sub, sub)
        a, d = a2[r, :], dy[r, :]
        gate, up = dot(a, wg[0]), dot(a, wu[0])
        dhid = dot_t(d, wd[0]).astype(BF).astype(F32)
        s = sigmoid(gate)
        accu[r, :] += dot_t((dhid * (gate * s)).astype(BF), wu[0])
        accg[r, :] += dot_t((dhid * up * (s * (1.0 + gate * (1.0 - s)))).astype(BF), wg[0])

    @pl.when(j == steps - 1)
    def _():
        da = (accg[...].astype(BF).astype(F32) + accu[...].astype(BF).astype(F32)).astype(BF).astype(F32)
        wide = h1[...].astype(F32)
        scale = lax.rsqrt(jnp.mean(wide * wide, -1, keepdims=True) + 1e-6)
        along = jnp.sum(da * wide, -1, keepdims=True) * (scale * scale * scale * (1.0 / wide.shape[-1]))
        dh1[...] = dy[...] + (da * scale - wide * along).astype(BF)
        gather.finish()
        for copy in part:
            copy.wait()


def gate_row(xb, rows):
    return xb * (2 * rows) + lax.div(xb, 2) * (4 * rows)


def gradient_kernel(
    n, rows,
    a2, a2s, dy, dys, a1, a1h, dh1, wg, wu, wd,
    og, ou, od, osq, dslots, b1,
    A, D, AT, DT, hid, dg, du, ag, au, ad, dT, wbuf, far, raw, keep, own, summed, frecv, rm, rp, GT, XR,
    lsem, wsem, gsend, grecv, bsend, brecv, rsend, rrecv, xsend, xrecv,
):
    t = pl.program_id(0)
    last = 2 * n - 1
    x, xa, xb_ = ring("x")
    y, ya, yb = ring("y")
    T, Dm = a2.shape
    half = T // 2
    ft = wbuf.shape[2]
    chunk = ft // SIDE
    top, bottom = pl.ds(0, half), pl.ds(half, half)
    gather = Gather(dh1, dslots, gsend, grecv)
    bcopy = lambda k, src, to: remote(src, b1.at[k], bsend.at[k], brecv.at[k], "x", to)
    rest = [bcopy(0, a1.at[bottom], xa), bcopy(1, a1.at[top], xb_), bcopy(2, a1h.at[0], xa), bcopy(3, a1h.at[1], xb_)]

    def weights(t):
        layer, j, slot = 1 - lax.div(t, n), lax.rem(t, n), lax.rem(t, 2)
        out = []
        for k in range(SIDE):
            at = pl.multiple_of(x * (n * ft) + k * ft + j * chunk, chunk)
            to = pl.ds(k * chunk, chunk)
            out.append(pltpu.make_async_copy(wg.at[layer, :, pl.ds(at, chunk)], wbuf.at[slot, 0, :, to], wsem.at[slot, 3 * k]))
            out.append(pltpu.make_async_copy(wu.at[layer, :, pl.ds(at, chunk)], wbuf.at[slot, 1, :, to], wsem.at[slot, 3 * k + 1]))
            out.append(pltpu.make_async_copy(wd.at[layer, pl.ds(at, chunk), :], wbuf.at[slot, 2, to, :], wsem.at[slot, 3 * k + 2]))
        return out

    def load(pairs):
        copies = [pltpu.make_async_copy(src, dst, lsem.at[k]) for k, (src, dst) in enumerate(pairs)]
        for copy in copies:
            copy.start()
        for copy in copies:
            copy.wait()

    def transpose():
        def one(s, _):
            AT[s] = A[s].T
            DT[s] = D[s].T
            return 0

        lax.fori_loop(0, SIDE, one, 0)

    def reduction(t):
        s = lax.rem(t, 3)
        h = far.shape[1] // 2
        lo, hi = pl.ds(0, h), pl.ds(h, h)
        c = lambda k, src, dst, to: remote(src, dst, rsend.at[s, k], rrecv.at[s, k], "y", to)
        return [
            c(0, far.at[s, lo], frecv.at[s, lo], ya),
            c(1, far.at[s, hi], frecv.at[s, hi], yb),
            c(2, raw.at[s, hi], rm.at[s, hi], ya),
            c(3, raw.at[s, lo], rp.at[s, lo], yb),
            c(4, summed.at[s, lo], rm.at[s, lo], ya),
            c(5, summed.at[s, hi], rp.at[s, hi], yb),
        ]

    def pack(t):
        s = lax.rem(t, 3)
        dT[...] = ad[...].T

        def rows_for(rel):
            yd = lax.rem(y + rel, SIDE)
            parts = {}
            for b in range(SIDE):
                at = pl.multiple_of(b * (SIDE * rows) + yd * rows, rows)
                to = b * 2 * rows + (b // 2) * 4 * rows
                parts[to] = ag[pl.ds(at, rows), :]
                parts[to + rows] = au[pl.ds(at, rows), :]
            at = pl.multiple_of(yd * chunk, chunk)
            parts[4 * rows] = dT[pl.ds(at, chunk // 2), :]
            parts[6 * rows] = dT[pl.ds(at + chunk // 2, chunk // 2), :]
            return parts

        h = far.shape[1] // 2
        for to, v in rows_for(2).items():
            far[s, pl.ds(to, v.shape[0]), :] = v.astype(BF)
        for to, v in rows_for(1).items():
            if to < h:
                keep[s, pl.ds(to, v.shape[0]), :] = v
            else:
                raw[s, pl.ds(to, v.shape[0]), :] = v.astype(BF)
        for to, v in rows_for(3).items():
            if to < h:
                raw[s, pl.ds(to, v.shape[0]), :] = v.astype(BF)
            else:
                keep[s, pl.ds(to, v.shape[0]), :] = v
        for to, v in rows_for(0).items():
            own[s, pl.ds(to, v.shape[0]), :] = v

    def total(t):
        s = lax.rem(t, 3)
        copies = reduction(t)
        copies[0].wait_recv()
        copies[1].wait_recv()
        summed[s] = (keep[s] + frecv[s].astype(F32)).astype(BF)
        copies[4].start()
        copies[5].start()

    def across(t):
        out = []
        for r in range(1, SIDE):
            to = lax.rem(x + r, SIDE)
            at = pl.multiple_of(gate_row(to, rows), 2 * rows)
            out.append(remote(GT.at[t, pl.ds(at, 2 * rows)], XR.at[t, r - 1], xsend.at[t, r - 1], xrecv.at[t, r - 1], "x", to))
        return out

    def final(t):
        s = lax.rem(t, 3)
        copies = reduction(t)
        for copy in copies[2:]:
            copy.wait_recv()
        for copy in copies:
            copy.wait_send()
        GT[t] = (own[s] + rm[s].astype(F32) + rp[s].astype(F32)).astype(BF)
        for copy in across(t):
            copy.start()

    def assemble(t):
        layer, j = 1 - lax.div(t, n), lax.rem(t, n)
        for copy in across(t):
            copy.wait()
        squares = jnp.zeros((8, 128), F32)
        for r in range(SIDE):
            source = lax.rem(x + SIDE - r, SIDE)
            if r:
                piece = XR[t, r - 1]
            else:
                piece = GT[t, pl.ds(pl.multiple_of(gate_row(x, rows), 2 * rows), 2 * rows), :]
            wide = piece.astype(F32)
            squares += fold(wide * wide)
            for k in range(SIDE):
                at = pl.multiple_of(source * (n * ft) + k * ft + j * chunk, chunk)
                og[layer, :, pl.ds(at, chunk)] = piece[:rows, k * chunk : (k + 1) * chunk]
                ou[layer, :, pl.ds(at, chunk)] = piece[rows:, k * chunk : (k + 1) * chunk]
        piece = GT[t, 4 * rows : 8 * rows, :]
        wide = piece.astype(F32)
        squares += fold(wide * wide)
        od[layer, pl.ds(pl.multiple_of(j * chunk, chunk), chunk), :] = piece
        osq[...] += squares

    @pl.when(t == 0)
    def _():
        greet([("x", xa), ("x", xb_), ("x", lax.rem(x + 2, SIDE)), ("y", ya), ("y", yb)])
        gather.start()
        for copy in rest:
            copy.start()
        for copy in weights(t):
            copy.start()
        osq[...] = jnp.zeros_like(osq)
        load([(a2, A.at[0]), (dy, D.at[0])] + [(a2s.at[k], A.at[k + 1]) for k in range(3)] + [(dys.at[k], D.at[k + 1]) for k in range(3)])
        transpose()

    @pl.when(t == n)
    def _():
        gather.finish()
        for copy in rest:
            copy.wait()
        load(
            [(a1, A.at[0]), (dh1, D.at[0])]
            + [(a1h.at[0], A.at[1, top]), (b1.at[0], A.at[1, bottom]), (b1.at[1], A.at[2, top]), (a1h.at[1], A.at[2, bottom])]
            + [(b1.at[2], A.at[3, top]), (b1.at[3], A.at[3, bottom])]
            + [(dslots.at[k], D.at[k + 1]) for k in range(3)]
        )
        transpose()

    for copy in weights(t):
        copy.wait()

    @pl.when(t < last)
    def _():
        for copy in weights(t + 1):
            copy.start()

    slot = lax.rem(t, 2)
    sub = half
    ag[...] = jnp.zeros_like(ag)
    au[...] = jnp.zeros_like(au)
    ad[...] = jnp.zeros_like(ad)

    def chain(s, b):
        for i in range(T // sub):
            r = pl.ds(i * sub, sub)
            a, d = A[s, r, :], D[s, r, :]
            gate, up = dot(a, wbuf[slot, 0]), dot(a, wbuf[slot, 1])
            dhid = dot_t(d, wbuf[slot, 2]).astype(BF).astype(F32)
            g = sigmoid(gate)
            silu = gate * g
            hid[b, r, :] = (silu * up).astype(BF)
            du[b, r, :] = (dhid * silu).astype(BF)
            dg[b, r, :] = (dhid * up * (g * (1.0 + gate * (1.0 - g)))).astype(BF)

    def contract(s, b):
        ag[...] += dot(AT[s], dg[b])
        au[...] += dot(AT[s], du[b])
        ad[...] += dot(DT[s], hid[b])

    for s in range(SIDE):
        chain(s, s % 2)
        if s:
            contract(s - 1, (s - 1) % 2)
    contract(SIDE - 1, (SIDE - 1) % 2)

    @pl.when(t == 0)
    def _():
        gather.relay()

    @pl.when(t >= 3)
    def _():
        assemble(t - 3)

    @pl.when(t >= 2)
    def _():
        final(t - 2)

    @pl.when(t >= 1)
    def _():
        total(t - 1)

    pack(t)
    for copy in reduction(t)[:4]:
        copy.start()

    @pl.when(t == last)
    def _():
        final(t - 1)
        total(t)
        assemble(t - 2)
        assemble(t - 1)
        final(t)
        assemble(t)


def fold(v):
    out = None
    for i in range(v.shape[0] // 8):
        for k in range(v.shape[1] // 128):
            tile = v[i * 8 : i * 8 + 8, k * 128 : k * 128 + 128]
            out = tile if out is None else out + tile
    return out


def squares_kernel(mine, out, got, send, recv):
    x, y = lax.axis_index("x"), lax.axis_index("y")
    peers = [(lax.rem(x + i, SIDE), lax.rem(y + j, SIDE)) for i in range(SIDE) for j in range(SIDE)][1:]
    barrier = pltpu.get_barrier_semaphore()
    for px, py in peers:
        pl.semaphore_signal(barrier, inc=1, device_id={"x": px, "y": py}, device_id_type=MESH)
    pl.semaphore_wait(barrier, len(peers))
    copies = [
        pltpu.make_async_remote_copy(
            src_ref=mine, dst_ref=got.at[k], send_sem=send.at[k], recv_sem=recv.at[k], device_id={"x": px, "y": py}, device_id_type=MESH
        )
        for k, (px, py) in enumerate(peers)
    ]
    for copy in copies:
        copy.start()
    for copy in copies:
        copy.wait()
    total = mine[...]
    for k in range(len(peers)):
        total += got[k]
    out[...] = total


def update_kernel(count, _, sq, *refs):
    g, m, v, w, nw, nm, nv = (refs[3 * i : 3 * i + 3] for i in range(7))
    factor = jnp.minimum(1.0, 0.5 * lax.rsqrt(jnp.sum(sq[...]) / count + 1e-30))
    for i in range(3):
        grad = g[i][...].astype(F32) * factor
        new_m = 0.9 * m[i][...] + 0.1 * grad
        new_v = 0.95 * v[i][...] + 0.05 * grad * grad
        wide = w[i][...].astype(F32)
        step = new_m * lax.rsqrt(new_v + 1e-8) + 0.1 * wide
        nw[i][...] = (wide - 0.02 * step).astype(BF)
        nm[i][...] = new_m
        nv[i][...] = new_v


def gather_kernel(bg, bu, bd, og, ou, od, local, send, recv):
    x, xa, xb = ring("x")
    y, ya, yb = ring("y")
    greet([("x", xa), ("x", xb), ("y", ya), ("y", yb)])
    colours = [("x", xa, "y", ya, -1), ("x", xb, "y", yb, 1), ("y", ya, "x", xa, -1), ("y", yb, "x", xb, 1)]
    blocks, outs = (bg, bu, bd), (og, ou, od)

    def owner(colour, i, j):
        first, _, _, _, back = colours[colour]
        i, j = (i, j) if first == "x" else (j, i)
        return lax.rem(x + SIDE + back * i, SIDE) * SIDE + lax.rem(y + SIDE + back * j, SIDE)

    def place(piece, colour, d):
        rows = blocks[piece].shape[1]
        at = pl.multiple_of(d * rows, rows)
        if piece < 2:
            width = bg.shape[2] // 4
            return outs[piece].at[:, pl.ds(at, rows), pl.ds(colour * width, width)]
        return outs[piece].at[:, pl.ds(at + colour * (rows // 4), rows // 4), :]

    def source(piece, colour, i, j):
        if i or j:
            return place(piece, colour, owner(colour, i, j))
        if piece < 2:
            width = bg.shape[2] // 4
            return blocks[piece].at[:, :, pl.ds(colour * width, width)]
        rows = bd.shape[1] // 4
        return bd.at[:, pl.ds(colour * rows, rows), :]

    def hop(piece, colour, i, j, along):
        a, an, b, bn, _ = colours[colour]
        i2, j2 = (i + 1, j) if along == 0 else (i, j + 1)
        return remote(
            source(piece, colour, i, j), place(piece, colour, owner(colour, i, j)),
            send.at[piece, colour, along], recv.at[piece, colour, i2 * SIDE + j2], a if along == 0 else b, an if along == 0 else bn,
        )

    mine = x * SIDE + y
    locals_ = []
    for piece in range(3):
        rows = blocks[piece].shape[1]
        locals_.append(pltpu.make_async_copy(blocks[piece], outs[piece].at[:, pl.ds(pl.multiple_of(mine * rows, rows), rows), :], local.at[piece]))
    events = sorted((12 * p + 3 * i + 4 * j, p, i, j) for p in range(3) for i in range(SIDE) for j in range(SIDE))
    sent = []
    for _, p, i, j in events:
        for c in range(4):
            if i or j:
                hop(p, c, i - 1 if j == 0 else i, j - 1 if j else 0, 0 if j == 0 else 1).wait_recv()
            if j == 0 and i < SIDE - 1:
                copy = hop(p, c, i, j, 0)
                copy.start()
                sent.append(copy)
            if j < SIDE - 1:
                copy = hop(p, c, i, j, 1)
                copy.start()
                sent.append(copy)
        if (p, i, j) == (0, 0, 0):
            for copy in locals_:
                copy.start()
    for copy in sent:
        copy.wait_send()
    for copy in locals_:
        copy.wait()


def params(limit, collective=None):
    if collective is None:
        return pltpu.CompilerParams(vmem_limit_bytes=limit)
    return pltpu.CompilerParams(vmem_limit_bytes=limit, collective_id=collective, has_side_effects=True)


def step(x, dy, wg, wu, wd, mg, mu, md, vg, vu, vd):
    x, dy = x[0], dy[0]
    T, Dm = x.shape
    layers, _, ff = wg.shape
    state = jax.ShapeDtypeStruct((T, Dm), BF)
    slots = jax.ShapeDtypeStruct((3, T, Dm), BF)
    whole = pl.BlockSpec((T, Dm), lambda j: (0, 0))

    def weight_specs(layer, ft):
        return [
            pl.BlockSpec((1, Dm, ft), lambda j: (layer, 0, j)),
            pl.BlockSpec((1, Dm, ft), lambda j: (layer, 0, j)),
            pl.BlockSpec((1, ft, Dm), lambda j: (layer, j, 0)),
        ]

    ft, sub = 1024, 512
    h1, a1, a2, dys = pl.pallas_call(
        functools.partial(forward_kernel, ff // ft, sub),
        grid=(ff // ft,),
        in_specs=[whole, ANY, *weight_specs(0, ft)],
        out_specs=[whole] * 3 + [ANY],
        out_shape=[state] * 3 + [slots],
        scratch_shapes=[pltpu.VMEM((T, Dm), F32), DMA((6,)), DMA((6,))],
        compiler_params=params(60 * MIB, 0),
        name="forward",
    )(x, dy, wg, wu, wd)

    ft, sub = 1024, 1024
    dh1, a2s, a1h = pl.pallas_call(
        functools.partial(own_kernel, ff // ft, sub),
        grid=(ff // ft,),
        in_specs=[whole] * 3 + [ANY] * 2 + weight_specs(1, ft),
        out_specs=[whole, ANY, ANY],
        out_shape=[state, slots, jax.ShapeDtypeStruct((2, T // 2, Dm), BF)],
        scratch_shapes=[pltpu.VMEM((T, Dm), F32)] * 2 + [DMA((6,)), DMA((6,)), DMA((2,)), DMA((2,))],
        compiler_params=params(60 * MIB, 1),
        name="own",
    )(h1, a2, dy, a2, a1, wg, wu, wd)

    ft = 512
    n = ff // (SIDE * ft)
    rows = mg.shape[1]
    piece = 2 * SIDE * rows + ft // SIDE
    vm = pltpu.VMEM
    full = lambda *shape: pl.BlockSpec(shape, lambda t: (0,) * len(shape))
    gg, gu, gd, sq, _, _ = pl.pallas_call(
        functools.partial(gradient_kernel, n, rows),
        grid=(layers * n,),
        in_specs=[ANY] * 10,
        out_specs=[full(*mg.shape), full(*mu.shape), full(*md.shape), full(8, 128), ANY, ANY],
        out_shape=[jax.ShapeDtypeStruct(m.shape, BF) for m in (mg, mu, md)]
        + [jax.ShapeDtypeStruct((8, 128), F32), slots, jax.ShapeDtypeStruct((4, T // 2, Dm), BF)],
        scratch_shapes=[vm((SIDE, T, Dm), BF)] * 2
        + [vm((SIDE, Dm, T), BF)] * 2
        + [vm((2, T, ft), BF)] * 3
        + [vm((Dm, ft), F32)] * 4
        + [vm((2, 3, ft, Dm), BF)]
        + [vm((3, piece, ft), BF)] * 2
        + [vm((3, piece, ft), F32)] * 2
        + [vm((3, piece, ft), BF)] * 4
        + [vm((2 * n, piece, ft), BF), vm((2 * n, 3, 2 * rows, ft), BF)]
        + [DMA((12,)), DMA((2, 12)), DMA((6,)), DMA((6,)), DMA((4,)), DMA((4,)), DMA((3, 6)), DMA((3, 6)), DMA((2 * n, 3)), DMA((2 * n, 3))],
        compiler_params=params(63 * MIB, 2),
        name="gradients",
    )(a2, a2s, dy, dys, a1, a1h, dh1, wg, wu, wd)

    tiny = pl.BlockSpec(memory_space=pltpu.VMEM)
    peers = SIDE * SIDE - 1
    sq = pl.pallas_call(
        squares_kernel,
        in_specs=[tiny],
        out_specs=tiny,
        out_shape=jax.ShapeDtypeStruct((8, 128), F32),
        scratch_shapes=[vm((peers, 8, 128), F32), DMA((peers,)), DMA((peers,))],
        compiler_params=params(8 * MIB, 3),
        name="squares",
    )(sq)

    count = sum(w.size for w in (wg, wu, wd))
    me = (lax.axis_index("x") * SIDE + lax.axis_index("y")).astype(jnp.int32).reshape(1)
    parts = 4
    across = (1, rows, ff // parts)
    down = (1, md.shape[1] // parts, Dm)
    wide = [pl.BlockSpec(across, lambda l, c, me: (l, 0, c))] * 2
    tall = [pl.BlockSpec(down, lambda l, c, me: (l, c, 0))]
    blocks = wide + tall
    of_weights = [pl.BlockSpec(across, lambda l, c, me: (l, me[0], c))] * 2 + [pl.BlockSpec(down, lambda l, c, me: (l, me[0] * parts + c, 0))]
    shapes = lambda dt: [jax.ShapeDtypeStruct(m.shape, dt) for m in (mg, mu, md)]
    bg, bu, bd, *moments = pl.pallas_call(
        functools.partial(update_kernel, count),
        grid_spec=pltpu.PrefetchScalarGridSpec(
            num_scalar_prefetch=1,
            grid=(layers, parts),
            in_specs=[pl.BlockSpec((8, 128), lambda l, c, me: (0, 0)), *blocks, *blocks, *blocks, *of_weights],
            out_specs=[*blocks, *blocks, *blocks],
        ),
        out_shape=shapes(BF) + shapes(F32) + shapes(F32),
        compiler_params=params(48 * MIB),
        name="update",
    )(me, sq, gg, gu, gd, mg, mu, md, vg, vu, vd, wg, wu, wd)

    new = pl.pallas_call(
        gather_kernel,
        in_specs=[tiny] * 3,
        out_specs=[ANY] * 3,
        out_shape=[jax.ShapeDtypeStruct(w.shape, BF) for w in (wg, wu, wd)],
        scratch_shapes=[DMA((3,)), DMA((3, 4, 2)), DMA((3, 4, SIDE * SIDE))],
        compiler_params=params(16 * MIB, 4),
        name="gather",
    )(bg, bu, bd)

    return (*new, *moments)


def solution(mesh):
    side = math.isqrt(mesh.shape["dp"])
    torus = Mesh(mesh.devices.reshape(-1, side, side), ("rep", "x", "y"))
    batch = P(("rep", "x", "y"))
    rows = P(None, ("x", "y"))
    out_rows = P("rep", ("x", "y"))
    return jax.shard_map(
        step,
        mesh=torus,
        in_specs=(batch, batch, P(), P(), P(), *[rows] * 6),
        out_specs=(P("rep"),) * 3 + (out_rows,) * 6,
        check_vma=False,
    )
```

```python
import functools
import math

import jax
import jax.numpy as jnp
from jax import lax
from jax.experimental import pallas as pl
from jax.experimental.pallas import tpu as pltpu
from jax.sharding import Mesh
from jax.sharding import PartitionSpec as P

F32, BF = jnp.float32, jnp.bfloat16
MESH = pl.DeviceIdType.MESH
MIB = 2**20
ANY = pl.BlockSpec(memory_space=pl.ANY)
DMA = pltpu.SemaphoreType.DMA
SIDE = 4


def dot(a, b):
    return jnp.dot(a, b, preferred_element_type=F32)


def dot_t(a, b):
    return lax.dot_general(a, b, (((1,), (1,)), ((), ())), preferred_element_type=F32)


def normed(h):
    wide = h.astype(F32)
    scale = lax.rsqrt(jnp.mean(wide * wide, -1, keepdims=True) + 1e-6)
    return (wide * scale).astype(BF)


def sigmoid(z):
    return 0.5 * jnp.tanh(0.5 * z) + 0.5


def ring(axis):
    me = lax.axis_index(axis)
    return me, lax.rem(me + 1, SIDE), lax.rem(me + SIDE - 1, SIDE)


def greet(peers):
    barrier = pltpu.get_barrier_semaphore()
    for axis, index in peers:
        pl.semaphore_signal(barrier, inc=1, device_id={axis: index}, device_id_type=MESH)
    pl.semaphore_wait(barrier, len(peers))


def remote(src, dst, send, recv, axis, index):
    return pltpu.make_async_remote_copy(
        src_ref=src, dst_ref=dst, send_sem=send, recv_sem=recv, device_id={axis: index}, device_id_type=MESH
    )


class Gather:
    def __init__(self, own, slots, send, recv):
        _, after, before = ring("x")
        half = own.shape[0] // 2
        top, bottom = pl.ds(0, half), pl.ds(half, half)
        c = lambda k, src, dst, to: remote(src, dst, send.at[k], recv.at[k], "x", to)
        self.first = [
            c(0, own.at[top], slots.at[0, top], after),
            c(1, own.at[bottom], slots.at[1, bottom], before),
            c(2, own.at[bottom], slots.at[0, bottom], after),
            c(3, own.at[top], slots.at[1, top], before),
        ]
        self.second = [
            c(4, slots.at[0, top], slots.at[2, top], after),
            c(5, slots.at[1, bottom], slots.at[2, bottom], before),
        ]

    def start(self):
        for copy in self.first:
            copy.start()

    def relay(self):
        for copy in self.first[:2]:
            copy.wait_recv()
        for copy in self.second:
            copy.start()

    def finish(self):
        for copy in self.first[2:] + self.second:
            copy.wait_recv()
        for copy in self.first + self.second:
            copy.wait_send()


def chain_kernel(
    steps, x, dy, dy_any, wg, wu, wd, a1, a2, dh1, dys, a2s, halves, h1, accg, accu, send, recv, send2, recv2, send1, recv1
):
    j = pl.program_id(0)
    _, after, before = ring("x")
    half = a1.shape[0] // 2
    gather_dy = Gather(dy_any, dys, send, recv)
    gather_a2 = Gather(a2, a2s, send2, recv2)
    part = [
        remote(a1.at[pl.ds(0, half)], halves.at[0], send1.at[0], recv1.at[0], "x", after),
        remote(a1.at[pl.ds(half, half)], halves.at[1], send1.at[1], recv1.at[1], "x", before),
    ]
    tiles = [pl.ds(k, 256) for k in range(0, wg.shape[2], 256)]

    @pl.when(j == 0)
    def _():
        greet([("x", after), ("x", before)])
        gather_dy.start()
        a1[...] = normed(x[...])
        accg[...] = jnp.zeros_like(accg)

    @pl.when(j == steps // 2)
    def _():
        gather_dy.relay()

    @pl.when(j == steps)
    def _():
        gather_a2.start()
        accg[...] = jnp.zeros_like(accg)
        accu[...] = jnp.zeros_like(accu)

    @pl.when(j == steps + 3)
    def _():
        gather_dy.finish()
        gather_a2.relay()
        for copy in part:
            copy.start()

    @pl.when(j < steps)
    def _():
        a = a1[...]
        hidden = []
        for k in tiles:
            gate, up = dot(a, wg[0, :, k]), dot(a, wu[0, :, k])
            hidden.append((gate * sigmoid(gate) * up).astype(BF))
        accg[...] += dot(jnp.concatenate(hidden, 1), wd[0])

    @pl.when(j == steps - 1)
    def _():
        h = x[...] + accg[...].astype(BF)
        h1[...] = h
        a2[...] = normed(h)

    @pl.when(j >= steps)
    def _():
        a, d = a2[...], dy[...]
        by_up, by_gate = [], []
        for k in tiles:
            gate, up = dot(a, wg[0, :, k]), dot(a, wu[0, :, k])
            dhid = dot_t(d, wd[0, k, :]).astype(BF).astype(F32)
            s = sigmoid(gate)
            silu = gate * s
            by_up.append((dhid * silu).astype(BF))
            by_gate.append((dhid * up * (s + silu * (1.0 - s))).astype(BF))
        accu[...] += dot_t(jnp.concatenate(by_up, 1), wu[0])
        accg[...] += dot_t(jnp.concatenate(by_gate, 1), wg[0])

    @pl.when(j == 2 * steps - 1)
    def _():
        da = (accg[...].astype(BF).astype(F32) + accu[...].astype(BF).astype(F32)).astype(BF).astype(F32)
        wide = h1[...].astype(F32)
        scale = lax.rsqrt(jnp.mean(wide * wide, -1, keepdims=True) + 1e-6)
        along = jnp.sum(da * wide, -1, keepdims=True) * (scale * scale * scale * (1.0 / wide.shape[-1]))
        dh1[...] = dy[...] + (da * scale - wide * along).astype(BF)
        gather_a2.finish()
        for copy in part:
            copy.wait()


def gate_row(xb, rows):
    return xb * (2 * rows) + lax.div(xb, 2) * (4 * rows)


def gradient_kernel(
    n, rows,
    a2, a2s, dy, dys, a1, a1h, dh1, wg, wu, wd,
    og, ou, od, osq, dslots, b1,
    A, D, AT, DT, hid, dg, du, silus, slopes, ag, au, ad, dT, wbuf, far, raw, keep, own, summed, frecv, rm, rp, GT, XR, others,
    lsem, wsem, gsend, grecv, bsend, brecv, rsend, rrecv, xsend, xrecv, qsend, qrecv,
):
    t = pl.program_id(0)
    last = 2 * n - 1
    x, xa, xb_ = ring("x")
    y, ya, yb = ring("y")
    T, Dm = a2.shape
    half = T // 2
    ft = wbuf.shape[2]
    chunk = ft // SIDE
    top, bottom = pl.ds(0, half), pl.ds(half, half)
    gather = Gather(dh1, dslots, gsend, grecv)
    bcopy = lambda k, src, to: remote(src, b1.at[k], bsend.at[k], brecv.at[k], "x", to)
    rest = [bcopy(0, a1.at[bottom], xa), bcopy(1, a1.at[top], xb_), bcopy(2, a1h.at[0], xa), bcopy(3, a1h.at[1], xb_)]

    def weights(t):
        layer, j, slot = 1 - lax.div(t, n), lax.rem(t, n), lax.rem(t, 2)
        out = []
        for k in range(SIDE):
            at = pl.multiple_of(x * (n * ft) + k * ft + j * chunk, chunk)
            to = pl.ds(k * chunk, chunk)
            out.append(pltpu.make_async_copy(wg.at[layer, :, pl.ds(at, chunk)], wbuf.at[slot, 0, :, to], wsem.at[slot, 3 * k]))
            out.append(pltpu.make_async_copy(wu.at[layer, :, pl.ds(at, chunk)], wbuf.at[slot, 1, :, to], wsem.at[slot, 3 * k + 1]))
            out.append(pltpu.make_async_copy(wd.at[layer, pl.ds(at, chunk), :], wbuf.at[slot, 2, to, :], wsem.at[slot, 3 * k + 2]))
        return out

    def loads(pairs):
        return [pltpu.make_async_copy(src, dst, lsem.at[k]) for k, (src, dst) in enumerate(pairs)]

    first = lambda: loads([(a2, A.at[0]), (dy, D.at[0])] + [(a2s.at[k], A.at[k + 1]) for k in range(3)] + [(dys.at[k], D.at[k + 1]) for k in range(3)])
    second = lambda: loads(
        [(a1, A.at[0]), (dh1, D.at[0])]
        + [(a1h.at[0], A.at[1, top]), (b1.at[0], A.at[1, bottom]), (b1.at[1], A.at[2, top]), (a1h.at[1], A.at[2, bottom])]
        + [(b1.at[2], A.at[3, top]), (b1.at[3], A.at[3, bottom])]
        + [(dslots.at[k], D.at[k + 1]) for k in range(3)]
    )

    def reduction(t):
        s = lax.rem(t, 3)
        h = far.shape[1] // 2
        lo, hi = pl.ds(0, h), pl.ds(h, h)
        c = lambda k, src, dst, to: remote(src, dst, rsend.at[s, k], rrecv.at[s, k], "y", to)
        return [
            c(0, far.at[s, lo], frecv.at[s, lo], ya),
            c(1, far.at[s, hi], frecv.at[s, hi], yb),
            c(2, raw.at[s, hi], rm.at[s, hi], ya),
            c(3, raw.at[s, lo], rp.at[s, lo], yb),
            c(4, summed.at[s, lo], rm.at[s, lo], ya),
            c(5, summed.at[s, hi], rp.at[s, hi], yb),
        ]

    def pack(t):
        s = lax.rem(t, 3)
        dT[...] = ad[...].T

        def rows_for(rel):
            yd = lax.rem(y + rel, SIDE)
            parts = {}
            for b in range(SIDE):
                at = pl.multiple_of(b * (SIDE * rows) + yd * rows, rows)
                to = b * 2 * rows + (b // 2) * 4 * rows
                parts[to] = ag[pl.ds(at, rows), :]
                parts[to + rows] = au[pl.ds(at, rows), :]
            at = pl.multiple_of(yd * chunk, chunk)
            parts[4 * rows] = dT[pl.ds(at, chunk // 2), :]
            parts[6 * rows] = dT[pl.ds(at + chunk // 2, chunk // 2), :]
            return parts

        h = far.shape[1] // 2
        for to, v in rows_for(2).items():
            far[s, pl.ds(to, v.shape[0]), :] = v.astype(BF)
        for to, v in rows_for(1).items():
            if to < h:
                keep[s, pl.ds(to, v.shape[0]), :] = v
            else:
                raw[s, pl.ds(to, v.shape[0]), :] = v.astype(BF)
        for to, v in rows_for(3).items():
            if to < h:
                raw[s, pl.ds(to, v.shape[0]), :] = v.astype(BF)
            else:
                keep[s, pl.ds(to, v.shape[0]), :] = v
        for to, v in rows_for(0).items():
            own[s, pl.ds(to, v.shape[0]), :] = v

    def total(t):
        s = lax.rem(t, 3)
        copies = reduction(t)
        copies[0].wait_recv()
        copies[1].wait_recv()
        summed[s] = (keep[s] + frecv[s].astype(F32)).astype(BF)
        copies[4].start()
        copies[5].start()

    def across(t):
        out, g = [], lax.rem(t, 4)
        for r in range(1, SIDE):
            to = lax.rem(x + r, SIDE)
            at = pl.multiple_of(gate_row(to, rows), 2 * rows)
            out.append(remote(GT.at[g, pl.ds(at, 2 * rows)], XR.at[g, r - 1], xsend.at[g, r - 1], xrecv.at[g, r - 1], "x", to))
        return out

    def final(t):
        s, g = lax.rem(t, 3), lax.rem(t, 4)
        copies = reduction(t)
        for copy in copies[2:]:
            copy.wait_recv()
        for copy in copies:
            copy.wait_send()
        mine = (own[s] + rm[s].astype(F32) + rp[s].astype(F32)).astype(BF)
        GT[g] = mine
        for copy in across(t):
            copy.start()
        wide = mine.astype(F32)
        osq[...] += fold(wide * wide)

    def assemble(t):
        layer, j, g = 1 - lax.div(t, n), lax.rem(t, n), lax.rem(t, 4)
        for copy in across(t):
            copy.wait()
        for r in range(SIDE):
            source = lax.rem(x + SIDE - r, SIDE)
            if r:
                piece = XR[g, r - 1]
            else:
                piece = GT[g, pl.ds(pl.multiple_of(gate_row(x, rows), 2 * rows), 2 * rows), :]
            for k in range(SIDE):
                at = pl.multiple_of(source * (n * ft) + k * ft + j * chunk, chunk)
                og[layer, :, pl.ds(at, chunk)] = piece[:rows, k * chunk : (k + 1) * chunk]
                ou[layer, :, pl.ds(at, chunk)] = piece[rows:, k * chunk : (k + 1) * chunk]
        od[layer, pl.ds(pl.multiple_of(j * chunk, chunk), chunk), :] = GT[g, 4 * rows : 8 * rows, :]

    peers = [(lax.rem(x + i, SIDE), lax.rem(y + k, SIDE)) for i in range(SIDE) for k in range(SIDE)][1:]

    @pl.when(t == 0)
    def _():
        for copy in first() + weights(t):
            copy.start()
        barrier = pltpu.get_barrier_semaphore()
        for px, py in peers:
            pl.semaphore_signal(barrier, inc=1, device_id={"x": px, "y": py}, device_id_type=MESH)
        pl.semaphore_wait(barrier, len(peers))
        gather.start()
        for copy in rest:
            copy.start()
        osq[...] = jnp.zeros_like(osq)
        for copy in first():
            copy.wait()

    @pl.when(t == n)
    def _():
        for copy in second():
            copy.wait()

    for copy in weights(t):
        copy.wait()

    @pl.when(t < last)
    def _():
        for copy in weights(t + 1):
            copy.start()

    slot = lax.rem(t, 2)
    sub = silus.shape[1]
    ag[...] = jnp.zeros_like(ag)
    au[...] = jnp.zeros_like(au)
    ad[...] = jnp.zeros_like(ad)

    def chain(s, b):
        AT[b] = A[s].T
        DT[b] = D[s].T
        for i in range(T // sub):
            r = pl.ds(i * sub, sub)
            a, d = A[s, r, :], D[s, r, :]
            for k in range(0, ft, 256):
                k = pl.ds(k, 256)
                gate = dot(a, wbuf[slot, 0, :, k])
                g = sigmoid(gate)
                silu = gate * g
                silus[b, :, k] = silu
                slopes[b, :, k] = g + silu * (1.0 - g)
                dhid = dot_t(d, wbuf[slot, 2, k, :]).astype(BF).astype(F32)
                du[b, r, k] = (dhid * silus[b, :, k]).astype(BF)
                slopes[b, :, k] = slopes[b, :, k] * dhid
                up = dot(a, wbuf[slot, 1, :, k])
                hid[b, r, k] = (silus[b, :, k] * up).astype(BF)
                dg[b, r, k] = (slopes[b, :, k] * up).astype(BF)

    def contract(b):
        ag[...] += dot(AT[b], dg[b])
        au[...] += dot(AT[b], du[b])
        ad[...] += dot(DT[b], hid[b])

    for s in range(SIDE):
        chain(s, s % 2)
        if s:
            contract((s - 1) % 2)
        if s == 1:
            pl.when(t >= 1)(functools.partial(total, t - 1))
    contract((SIDE - 1) % 2)

    @pl.when(t == n - 1)
    def _():
        gather.finish()
        for copy in rest:
            copy.wait()
        for copy in second():
            copy.start()

    @pl.when(t == 0)
    def _():
        gather.relay()

    @pl.when(t >= 3)
    def _():
        assemble(t - 3)

    @pl.when(t >= 2)
    def _():
        final(t - 2)

    pack(t)
    for copy in reduction(t)[:4]:
        copy.start()

    @pl.when(t == last)
    def _():
        final(t - 1)
        total(t)
        assemble(t - 2)
        final(t)
        copies = [
            pltpu.make_async_remote_copy(
                src_ref=osq, dst_ref=others.at[k], send_sem=qsend.at[k], recv_sem=qrecv.at[k], device_id={"x": px, "y": py}, device_id_type=MESH
            )
            for k, (px, py) in enumerate(peers)
        ]
        for copy in copies:
            copy.start()
        assemble(t - 1)
        assemble(t)
        for copy in copies:
            copy.wait()
        total_squares = osq[...]
        for k in range(len(peers)):
            total_squares += others[k]
        osq[...] = total_squares


def fold(v):
    out = None
    for i in range(v.shape[0] // 8):
        for k in range(v.shape[1] // 128):
            tile = v[i * 8 : i * 8 + 8, k * 128 : k * 128 + 128]
            out = tile if out is None else out + tile
    return out


def update_kernel(count, parts, sq, *refs):
    g, m, v, w, nw, nm, nv, bm, bv, bw = (refs[3 * i : 3 * i + 3] for i in range(10))
    came, left = refs[30:]
    mine = lax.axis_index("x") * SIDE + lax.axis_index("y")
    pieces = [(i, l, c) for i in range(3) for l in range(g[0].shape[0]) for c in range(parts)]

    def at(i, l, c, first=0):
        _, rows, width = g[i].shape
        if i < 2:
            return (l, pl.ds(first, rows), pl.ds(c * (width // parts), width // parts))
        return (l, pl.ds(first + c * (rows // parts), rows // parts), slice(None))

    def arrivals(k):
        i, l, c = pieces[k]
        here = at(i, l, c)
        there = at(i, l, c, pl.multiple_of(mine * g[i].shape[1], g[i].shape[1]))
        return [
            pltpu.make_async_copy(m[i].at[here], bm[i].at[here], came.at[k, 0]),
            pltpu.make_async_copy(v[i].at[here], bv[i].at[here], came.at[k, 1]),
            pltpu.make_async_copy(w[i].at[there], bw[i].at[here], came.at[k, 2]),
        ]

    def departures(k):
        i, l, c = pieces[k]
        here = at(i, l, c)
        return [
            pltpu.make_async_copy(bm[i].at[here], nm[i].at[here], left.at[k, 0]),
            pltpu.make_async_copy(bv[i].at[here], nv[i].at[here], left.at[k, 1]),
        ]

    for k in range(len(pieces)):
        for copy in arrivals(k):
            copy.start()
    factor = jnp.minimum(1.0, 0.5 * lax.rsqrt(jnp.sum(sq[...], keepdims=True) / count + 1e-30))
    for k, (i, l, c) in enumerate(pieces):
        here = at(i, l, c)
        for copy in arrivals(k):
            copy.wait()
        grad = g[i][here].astype(F32) * factor
        new_m = 0.9 * bm[i][here] + 0.1 * grad
        new_v = 0.95 * bv[i][here] + 0.05 * grad * grad
        wide = bw[i][here].astype(F32)
        step = new_m * lax.rsqrt(new_v + 1e-8) + 0.1 * wide
        nw[i][here] = (wide - 0.02 * step).astype(BF)
        bm[i][here] = new_m
        bv[i][here] = new_v
        for copy in departures(k):
            copy.start()
    for k in range(len(pieces)):
        for copy in departures(k):
            copy.wait()


def gather_kernel(bg, bu, bd, og, ou, od, local, send, recv):
    x, xa, xb = ring("x")
    y, ya, yb = ring("y")
    greet([("x", xa), ("x", xb), ("y", ya), ("y", yb)])
    colours = [("x", xa, "y", ya, -1), ("x", xb, "y", yb, 1), ("y", ya, "x", xa, -1), ("y", yb, "x", xb, 1)]
    blocks, outs = (bg, bu, bd), (og, ou, od)

    def owner(colour, i, j):
        first, _, _, _, back = colours[colour]
        i, j = (i, j) if first == "x" else (j, i)
        return lax.rem(x + SIDE + back * i, SIDE) * SIDE + lax.rem(y + SIDE + back * j, SIDE)

    def place(piece, colour, d):
        rows = blocks[piece].shape[1]
        at = pl.multiple_of(d * rows, rows)
        if piece < 2:
            width = bg.shape[2] // 4
            return outs[piece].at[:, pl.ds(at, rows), pl.ds(colour * width, width)]
        return outs[piece].at[:, pl.ds(at + colour * (rows // 4), rows // 4), :]

    def source(piece, colour, i, j):
        if i or j:
            return place(piece, colour, owner(colour, i, j))
        if piece < 2:
            width = bg.shape[2] // 4
            return blocks[piece].at[:, :, pl.ds(colour * width, width)]
        rows = bd.shape[1] // 4
        return bd.at[:, pl.ds(colour * rows, rows), :]

    def hop(piece, colour, i, j, along):
        a, an, b, bn, _ = colours[colour]
        i2, j2 = (i + 1, j) if along == 0 else (i, j + 1)
        return remote(
            source(piece, colour, i, j), place(piece, colour, owner(colour, i, j)),
            send.at[piece, colour, along], recv.at[piece, colour, i2 * SIDE + j2], a if along == 0 else b, an if along == 0 else bn,
        )

    mine = x * SIDE + y
    locals_ = []
    for piece in range(3):
        rows = blocks[piece].shape[1]
        locals_.append(pltpu.make_async_copy(blocks[piece], outs[piece].at[:, pl.ds(pl.multiple_of(mine * rows, rows), rows), :], local.at[piece]))
    events = sorted((12 * p + 3 * i + 4 * j, p, i, j) for p in range(3) for i in range(SIDE) for j in range(SIDE))
    sent = []
    for _, p, i, j in events:
        for c in range(4):
            if i or j:
                hop(p, c, i - 1 if j == 0 else i, j - 1 if j else 0, 0 if j == 0 else 1).wait_recv()
            if j == 0 and i < SIDE - 1:
                copy = hop(p, c, i, j, 0)
                copy.start()
                sent.append(copy)
            if j < SIDE - 1:
                copy = hop(p, c, i, j, 1)
                copy.start()
                sent.append(copy)
        if (p, i, j) == (0, 0, 0):
            for copy in locals_:
                copy.start()
    for copy in sent:
        copy.wait_send()
    for copy in locals_:
        copy.wait()


def out_kernel(src, dst, sem):
    part = src.shape[1] // 4
    copies = []
    for k in range(2 * 4):
        at = (k // 4, pl.ds(k % 4 * part, part))
        copies.append(pltpu.make_async_copy(src.at[at], dst.at[at], sem.at[k]))
    for copy in copies:
        copy.start()
    for copy in copies:
        copy.wait()


def cost(units, w):
    return pl.CostEstimate(flops=units * 2 * 1024 * w.shape[1] * w.shape[2], bytes_accessed=4 * w.size, transcendentals=0)


def params(limit, collective=None):
    if collective is None:
        return pltpu.CompilerParams(vmem_limit_bytes=limit)
    return pltpu.CompilerParams(vmem_limit_bytes=limit, collective_id=collective, has_side_effects=True)


def step(x, dy, wg, wu, wd, mg, mu, md, vg, vu, vd):
    x, dy = x[0], dy[0]
    T, Dm = x.shape
    layers, _, ff = wg.shape
    state = jax.ShapeDtypeStruct((T, Dm), BF)
    slots = jax.ShapeDtypeStruct((3, T, Dm), BF)
    whole = pl.BlockSpec((T, Dm), lambda j: (0, 0))

    tiny = pl.BlockSpec(memory_space=pltpu.VMEM)
    ft = 1024
    steps = ff // ft
    across = pl.BlockSpec((1, Dm, ft), lambda j: (lax.div(j, steps), 0, lax.rem(j, steps)))
    down = pl.BlockSpec((1, ft, Dm), lambda j: (lax.div(j, steps), lax.rem(j, steps), 0))
    a1, a2, dh1, dys, a2s, a1h = pl.pallas_call(
        functools.partial(chain_kernel, steps),
        grid=(layers * steps,),
        in_specs=[whole, whole, ANY, across, across, down],
        out_specs=[whole] * 3 + [ANY] * 3,
        out_shape=[state] * 3 + [slots] * 2 + [jax.ShapeDtypeStruct((2, T // 2, Dm), BF)],
        scratch_shapes=[pltpu.VMEM((T, Dm), BF), pltpu.VMEM((T, Dm), F32), pltpu.VMEM((T, Dm), F32)] + [DMA((6,))] * 4 + [DMA((2,))] * 2,
        compiler_params=params(60 * MIB, 0),
        cost_estimate=cost(8, wg),
        name="chain",
    )(x, dy, dy, wg, wu, wd)

    ft = 512
    n = ff // (SIDE * ft)
    rows = mg.shape[1]
    piece = 2 * SIDE * rows + ft // SIDE
    vm = pltpu.VMEM
    peers = SIDE * SIDE - 1
    full = lambda *shape: pl.BlockSpec(shape, lambda t: (0,) * len(shape))
    gg, gu, gd, sq, _, _ = pl.pallas_call(
        functools.partial(gradient_kernel, n, rows),
        grid=(layers * n,),
        in_specs=[ANY] * 10,
        out_specs=[tiny] * 4 + [ANY, ANY],
        out_shape=[pltpu.VMEM(m.shape, BF) for m in (mg, mu, md)]
        + [pltpu.VMEM((8, 128), F32), slots, jax.ShapeDtypeStruct((4, T // 2, Dm), BF)],
        scratch_shapes=[vm((SIDE, T, Dm), BF)] * 2
        + [vm((2, Dm, T), BF)] * 2
        + [vm((2, T, ft), BF)] * 3
        + [vm((2, 256, ft), F32)] * 2
        + [vm((Dm, ft), F32)] * 4
        + [vm((2, 3, ft, Dm), BF)]
        + [vm((3, piece, ft), BF)] * 2
        + [vm((3, piece, ft), F32)] * 2
        + [vm((3, piece, ft), BF)] * 4
        + [vm((4, piece, ft), BF), vm((4, 3, 2 * rows, ft), BF), vm((peers, 8, 128), F32)]
        + [DMA((12,)), DMA((2, 12)), DMA((6,)), DMA((6,)), DMA((4,)), DMA((4,)), DMA((3, 6)), DMA((3, 6)), DMA((4, 3)), DMA((4, 3)), DMA((peers,)), DMA((peers,))],
        compiler_params=params(59 * MIB, 1),
        cost_estimate=cost(12, wg),
        name="gradients",
    )(a2, a2s, dy, dys, a1, a1h, dh1, wg, wu, wd)

    count = sum(w.size for w in (wg, wu, wd))
    parts = 4
    shapes = lambda dt: [jax.ShapeDtypeStruct(m.shape, dt) for m in (mg, mu, md)]
    buffers = lambda dt: [vm(m.shape, dt) for m in (mg, mu, md)]
    bg, bu, bd, *moments = pl.pallas_call(
        functools.partial(update_kernel, count, parts),
        in_specs=[tiny] * 4 + [ANY] * 9,
        out_specs=[tiny] * 3 + [ANY] * 6,
        out_shape=buffers(BF) + shapes(F32) + shapes(F32),
        scratch_shapes=buffers(F32) + buffers(F32) + buffers(BF) + [DMA((3 * layers * parts, 3)), DMA((3 * layers * parts, 2))],
        compiler_params=params(46 * MIB),
        name="update",
    )(sq, gg, gu, gd, mg, mu, md, vg, vu, vd, wg, wu, wd)

    new = pl.pallas_call(
        gather_kernel,
        in_specs=[ANY] * 3,
        out_specs=[tiny] * 3,
        out_shape=[pltpu.VMEM(w.shape, BF) for w in (wg, wu, wd)],
        scratch_shapes=[DMA((3,)), DMA((3, 4, 2)), DMA((3, 4, SIDE * SIDE))],
        compiler_params=params(MIB, 2),
        cost_estimate=cost(24, wg),
        name="gather",
    )(bg, bu, bd)

    new = [
        pl.pallas_call(
            out_kernel,
            in_specs=[tiny],
            out_specs=ANY,
            out_shape=jax.ShapeDtypeStruct(w.shape, BF),
            scratch_shapes=[DMA((8,))],
            compiler_params=params(MIB),
            name="out",
        )(w)
        for w in new
    ]
    return (*new, *moments)


def solution(mesh):
    side = math.isqrt(mesh.shape["dp"])
    torus = Mesh(mesh.devices.reshape(-1, side, side), ("rep", "x", "y"))
    batch = P(("rep", "x", "y"))
    rows = P(None, ("x", "y"))
    out_rows = P("rep", ("x", "y"))
    return jax.shard_map(
        step,
        mesh=torus,
        in_specs=(batch, batch, P(), P(), P(), *[rows] * 6),
        out_specs=(P("rep"),) * 3 + (out_rows,) * 6,
        check_vma=False,
    )
```

```python
import functools
import math

import jax
import jax.numpy as jnp
from jax import lax
from jax.experimental import pallas as pl
from jax.experimental.pallas import tpu as pltpu
from jax.sharding import Mesh
from jax.sharding import PartitionSpec as P

F32, BF = jnp.float32, jnp.bfloat16
MESH = pl.DeviceIdType.MESH
MIB = 2**20
ANY = pl.BlockSpec(memory_space=pl.ANY)
DMA = pltpu.SemaphoreType.DMA
SIDE = 4


def dot(a, b):
    return jnp.dot(a, b, preferred_element_type=F32)


def dot_t(a, b):
    return lax.dot_general(a, b, (((1,), (1,)), ((), ())), preferred_element_type=F32)


def normed(h):
    wide = h.astype(F32)
    scale = lax.rsqrt(jnp.mean(wide * wide, -1, keepdims=True) + 1e-6)
    return (wide * scale).astype(BF)


def sigmoid(z):
    return 0.5 * jnp.tanh(0.5 * z) + 0.5


def ring(axis):
    me = lax.axis_index(axis)
    return me, lax.rem(me + 1, SIDE), lax.rem(me + SIDE - 1, SIDE)


class Place:
    def __init__(self):
        self.turned = lax.rem(lax.axis_index("rep"), 2)
        x, y = lax.axis_index("x"), lax.axis_index("y")
        self.u, self.v = self.pair(x, y)

    def pair(self, a, b):
        return a + self.turned * (b - a), b + self.turned * (a - b)

    def device(self, u, v):
        x, y = self.pair(u, v)
        return {"x": x, "y": y}

    def rank(self, u, v):
        x, y = self.pair(u, v)
        return x * SIDE + y

    def gathering(self, step):
        return self.device(lax.rem(self.u + step, SIDE), self.v)

    def summing(self, step):
        return self.device(self.u, lax.rem(self.v + step, SIDE))


def greet(devices):
    barrier = pltpu.get_barrier_semaphore()
    for device in devices:
        pl.semaphore_signal(barrier, inc=1, device_id=device, device_id_type=MESH)
    pl.semaphore_wait(barrier, len(devices))


def remote(src, dst, send, recv, device):
    return pltpu.make_async_remote_copy(
        src_ref=src, dst_ref=dst, send_sem=send, recv_sem=recv, device_id=device, device_id_type=MESH
    )


class Gather:
    def __init__(self, place, own, slots, send, recv):
        after, before = place.gathering(1), place.gathering(SIDE - 1)
        half = own.shape[0] // 2
        top, bottom = pl.ds(0, half), pl.ds(half, half)
        c = lambda k, src, dst, to: remote(src, dst, send.at[k], recv.at[k], to)
        self.first = [
            c(0, own.at[top], slots.at[0, top], after),
            c(1, own.at[bottom], slots.at[1, bottom], before),
            c(2, own.at[bottom], slots.at[0, bottom], after),
            c(3, own.at[top], slots.at[1, top], before),
        ]
        self.second = [
            c(4, slots.at[0, top], slots.at[2, top], after),
            c(5, slots.at[1, bottom], slots.at[2, bottom], before),
        ]

    def start(self):
        for copy in self.first:
            copy.start()

    def relay(self):
        for copy in self.first[:2]:
            copy.wait_recv()
        for copy in self.second:
            copy.start()

    def finish(self):
        for copy in self.first[2:] + self.second:
            copy.wait_recv()
        for copy in self.first + self.second:
            copy.wait_send()


def chain_kernel(
    steps, x, dy, dy_any, wg_any, wu_any, wd_any, a1, a2, dh1, dys, a2s, halves, saved, h1, accg, accu, bg, bu, bd,
    stage, wsem, ssem, send, recv, send2, recv2, send1, recv1,
):
    j = pl.program_id(0)
    place = Place()
    after, before = place.gathering(1), place.gathering(SIDE - 1)
    half = a1.shape[0] // 2
    gather_dy = Gather(place, dy_any, dys, send, recv)
    gather_a2 = Gather(place, a2, a2s, send2, recv2)
    part = [
        remote(a1.at[pl.ds(0, half)], halves.at[0], send1.at[0], recv1.at[0], after),
        remote(a1.at[pl.ds(half, half)], halves.at[1], send1.at[1], recv1.at[1], before),
    ]
    ft = bg.shape[2]
    tiles = [pl.ds(q, 256) for q in range(0, ft, 256)]

    width = saved.shape[2] // SIDE
    begin = lax.div(place.rank(place.u, 0), ft // width)

    def share(k):
        return lax.rem(k + begin, steps)

    def weights(j):
        layer, slot = lax.div(j, steps), lax.rem(j, 2)
        step = lax.rem(j + layer * begin, steps)
        at = pl.ds(pl.multiple_of(step * ft, ft), ft)
        return [
            pltpu.make_async_copy(wg_any.at[layer, :, at], bg.at[slot], wsem.at[slot, 0]),
            pltpu.make_async_copy(wu_any.at[layer, :, at], bu.at[slot], wsem.at[slot, 1]),
            pltpu.make_async_copy(wd_any.at[layer, at, :], bd.at[slot], wsem.at[slot, 2]),
        ]

    @pl.when(j == 0)
    def _():
        for copy in weights(j):
            copy.start()
        greet([after, before])
        gather_dy.start()
        a1[...] = normed(x[...])
        accg[...] = jnp.zeros_like(accg)

    @pl.when(j == steps // 2)
    def _():
        gather_dy.relay()

    @pl.when(j == steps)
    def _():
        gather_a2.start()
        accg[...] = jnp.zeros_like(accg)
        accu[...] = jnp.zeros_like(accu)

    @pl.when(j == steps + 3)
    def _():
        gather_dy.finish()
        gather_a2.relay()
        for copy in part:
            copy.start()

    k = j - steps

    def kept(k, do):
        for part in range(ft // width):
            block = share(k) * (ft // width) + part
            u, v = place.pair(lax.div(block, SIDE), lax.rem(block, SIDE))
            to = pl.ds(pl.multiple_of(v * width, width), width)

            @pl.when((k >= 0) & (u == place.u))
            def _():
                slot = lax.rem(k, 2)
                do(pltpu.make_async_copy(stage.at[slot, :, :, pl.ds(part * width, width)], saved.at[:, :, to], ssem.at[slot, part]))

    kept(k - 2, lambda copy: copy.wait())

    for copy in weights(j):
        copy.wait()

    @pl.when(j < 2 * steps - 1)
    def _():
        for copy in weights(j + 1):
            copy.start()

    slot = lax.rem(j, 2)
    wg, wu, wd = bg.at[pl.ds(slot, 1)], bu.at[pl.ds(slot, 1)], bd.at[pl.ds(slot, 1)]

    @pl.when(j < steps)
    def _():
        a = a1[...]
        hidden = []
        for q in tiles:
            gate, up = dot(a, wg[0, :, q]), dot(a, wu[0, :, q])
            hidden.append((gate * sigmoid(gate) * up).astype(BF))
        accg[...] += dot(jnp.concatenate(hidden, 1), wd[0])

    @pl.when(j == steps - 1)
    def _():
        h = x[...] + accg[...].astype(BF)
        h1[...] = h
        a2[...] = normed(h)

    @pl.when(j >= steps)
    def _():
        a, d = a2[...], dy[...]
        for q in tiles:
            gate, up = dot(a, wg[0, :, q]), dot(a, wu[0, :, q])
            dhid = dot_t(d, wd[0, q, :]).astype(BF).astype(F32)
            s = sigmoid(gate)
            silu = gate * s
            stage[slot, 0, :, q] = (silu * up).astype(BF)
            stage[slot, 1, :, q] = (dhid * silu).astype(BF)
            stage[slot, 2, :, q] = (dhid * up * (s + silu * (1.0 - s))).astype(BF)
        accu[...] += dot_t(stage[slot, 1], wu[0])
        accg[...] += dot_t(stage[slot, 2], wg[0])

    kept(k, lambda copy: copy.start())

    @pl.when(j == 2 * steps - 1)
    def _():
        da = (accg[...].astype(BF).astype(F32) + accu[...].astype(BF).astype(F32)).astype(BF).astype(F32)
        wide = h1[...].astype(F32)
        scale = lax.rsqrt(jnp.mean(wide * wide, -1, keepdims=True) + 1e-6)
        along = jnp.sum(da * wide, -1, keepdims=True) * (scale * scale * scale * (1.0 / wide.shape[-1]))
        dh1[...] = dy[...] + (da * scale - wide * along).astype(BF)
        for back in (1, 0):
            kept(k - back, lambda copy: copy.wait())
        gather_a2.finish()
        for copy in part:
            copy.wait()


def gate_row(xb, rows):
    return xb * (2 * rows) + lax.div(xb, 2) * (4 * rows)


def gradient_kernel(
    n, rows,
    a2, a2s, dy, dys, a1, a1h, dh1, wg, wu, wd, saved,
    og, ou, od, osq, dslots, b1,
    A, D, AT, DT, hid, dg, du, silus, slopes, ag, au, ad, dT, wbuf, far, raw, keep, own, summed, frecv, rm, rp, GT, XR, others, factors,
    lsem, fsem, wsem, gsend, grecv, bsend, brecv, rsend, rrecv, xsend, xrecv, qsend, qrecv,
):
    t = pl.program_id(0)
    last = 2 * n - 1
    place = Place()
    u, v = place.u, place.v
    after, before = place.gathering(1), place.gathering(SIDE - 1)
    T, Dm = a2.shape
    half = T // 2
    ft = wbuf.shape[2]
    chunk = ft // SIDE
    top, bottom = pl.ds(0, half), pl.ds(half, half)
    gather = Gather(place, dh1, dslots, gsend, grecv)
    bcopy = lambda k, src, to: remote(src, b1.at[k], bsend.at[k], brecv.at[k], to)
    rest = [bcopy(0, a1.at[bottom], after), bcopy(1, a1.at[top], before), bcopy(2, a1h.at[0], after), bcopy(3, a1h.at[1], before)]

    def weights(t):
        layer, j, slot = 1 - lax.div(t, n), lax.rem(t, n), lax.rem(t, 2)
        out = []
        for k in range(SIDE):
            at = pl.multiple_of(place.rank(u, k) * (n * chunk) + j * chunk, chunk)
            to = pl.ds(k * chunk, chunk)
            out.append(pltpu.make_async_copy(wg.at[layer, :, pl.ds(at, chunk)], wbuf.at[slot, 0, :, to], wsem.at[slot, 3 * k]))
            out.append(pltpu.make_async_copy(wu.at[layer, :, pl.ds(at, chunk)], wbuf.at[slot, 1, :, to], wsem.at[slot, 3 * k + 1]))
            out.append(pltpu.make_async_copy(wd.at[layer, pl.ds(at, chunk), :], wbuf.at[slot, 2, to, :], wsem.at[slot, 3 * k + 2]))
        return out

    def loads(pairs):
        return [pltpu.make_async_copy(src, dst, lsem.at[k]) for k, (src, dst) in enumerate(pairs)]

    first = lambda: loads([(a2, A.at[0]), (dy, D.at[0])] + [(a2s.at[k], A.at[k + 1]) for k in range(3)] + [(dys.at[k], D.at[k + 1]) for k in range(3)])
    second = lambda: loads(
        [(a1, A.at[0]), (dh1, D.at[0])]
        + [(a1h.at[0], A.at[1, top]), (b1.at[0], A.at[1, bottom]), (b1.at[1], A.at[2, top]), (a1h.at[1], A.at[2, bottom])]
        + [(b1.at[2], A.at[3, top]), (b1.at[3], A.at[3, bottom])]
        + [(dslots.at[k], D.at[k + 1]) for k in range(3)]
    )

    def own_factors(t):
        out = []
        for k in range(SIDE):
            at = pl.multiple_of(k * (n * chunk) + t * chunk, chunk)
            out.append(pltpu.make_async_copy(saved.at[:, :, pl.ds(at, chunk)], factors.at[:, :, pl.ds(k * chunk, chunk)], fsem.at[k]))
        return out

    def reduction(t):
        s = lax.rem(t, 3)
        h = far.shape[1] // 2
        lo, hi = pl.ds(0, h), pl.ds(h, h)
        next_, last_ = place.summing(1), place.summing(SIDE - 1)
        c = lambda k, src, dst, to: remote(src, dst, rsend.at[s, k], rrecv.at[s, k], to)
        return [
            c(0, far.at[s, lo], frecv.at[s, lo], next_),
            c(1, far.at[s, hi], frecv.at[s, hi], last_),
            c(2, raw.at[s, hi], rm.at[s, hi], next_),
            c(3, raw.at[s, lo], rp.at[s, lo], last_),
            c(4, summed.at[s, lo], rm.at[s, lo], next_),
            c(5, summed.at[s, hi], rp.at[s, hi], last_),
        ]

    def pack(t):
        s = lax.rem(t, 3)
        dT[...] = ad[...].T

        def rows_for(rel):
            vd = lax.rem(v + rel, SIDE)
            parts = {}
            for b in range(SIDE):
                at = pl.multiple_of(place.rank(b, vd) * rows, rows)
                to = b * 2 * rows + (b // 2) * 4 * rows
                parts[to] = ag[pl.ds(at, rows), :]
                parts[to + rows] = au[pl.ds(at, rows), :]
            at = pl.multiple_of(vd * chunk, chunk)
            parts[4 * rows] = dT[pl.ds(at, chunk // 2), :]
            parts[6 * rows] = dT[pl.ds(at + chunk // 2, chunk // 2), :]
            return parts

        h = far.shape[1] // 2
        for to, part in rows_for(2).items():
            far[s, pl.ds(to, part.shape[0]), :] = part.astype(BF)
        for to, part in rows_for(1).items():
            if to < h:
                keep[s, pl.ds(to, part.shape[0]), :] = part
            else:
                raw[s, pl.ds(to, part.shape[0]), :] = part.astype(BF)
        for to, part in rows_for(3).items():
            if to < h:
                raw[s, pl.ds(to, part.shape[0]), :] = part.astype(BF)
            else:
                keep[s, pl.ds(to, part.shape[0]), :] = part
        for to, part in rows_for(0).items():
            own[s, pl.ds(to, part.shape[0]), :] = part

    def total(t):
        s = lax.rem(t, 3)
        copies = reduction(t)
        copies[0].wait_recv()
        copies[1].wait_recv()
        summed[s] = (keep[s] + frecv[s].astype(F32)).astype(BF)
        copies[4].start()
        copies[5].start()

    def across(t):
        out, g = [], lax.rem(t, 4)
        for r in range(1, SIDE):
            to = lax.rem(u + r, SIDE)
            at = pl.multiple_of(gate_row(to, rows), 2 * rows)
            out.append(remote(GT.at[g, pl.ds(at, 2 * rows)], XR.at[g, r - 1], xsend.at[g, r - 1], xrecv.at[g, r - 1], place.device(to, v)))
        return out

    def final(t):
        s, g = lax.rem(t, 3), lax.rem(t, 4)
        copies = reduction(t)
        for copy in copies[2:]:
            copy.wait_recv()
        for copy in copies:
            copy.wait_send()
        mine = (own[s] + rm[s].astype(F32) + rp[s].astype(F32)).astype(BF)
        GT[g] = mine
        for copy in across(t):
            copy.start()
        wide = mine.astype(F32)
        osq[...] += fold(wide * wide)

    def assemble(t):
        layer, j, g = 1 - lax.div(t, n), lax.rem(t, n), lax.rem(t, 4)
        for copy in across(t):
            copy.wait()
        for r in range(SIDE):
            source = lax.rem(u + SIDE - r, SIDE)
            if r:
                piece = XR[g, r - 1]
            else:
                piece = GT[g, pl.ds(pl.multiple_of(gate_row(u, rows), 2 * rows), 2 * rows), :]
            for k in range(SIDE):
                at = pl.multiple_of(place.rank(source, k) * (n * chunk) + j * chunk, chunk)
                og[layer, :, pl.ds(at, chunk)] = piece[:rows, k * chunk : (k + 1) * chunk]
                ou[layer, :, pl.ds(at, chunk)] = piece[rows:, k * chunk : (k + 1) * chunk]
        od[layer, pl.ds(pl.multiple_of(j * chunk, chunk), chunk), :] = GT[g, 4 * rows : 8 * rows, :]

    peers = [place.device(lax.rem(u + i, SIDE), lax.rem(v + k, SIDE)) for i in range(SIDE) for k in range(SIDE)][1:]

    @pl.when(t == 0)
    def _():
        for copy in first() + weights(t) + own_factors(t):
            copy.start()
        greet(peers)
        gather.start()
        for copy in rest:
            copy.start()
        osq[...] = jnp.zeros_like(osq)
        for copy in first():
            copy.wait()

    @pl.when(t == n)
    def _():
        for copy in second():
            copy.wait()

    for copy in weights(t):
        copy.wait()

    @pl.when(t < last)
    def _():
        for copy in weights(t + 1):
            copy.start()

    slot = lax.rem(t, 2)
    sub = silus.shape[1]
    def chain(s, b):
        AT[b] = A[s].T
        DT[b] = D[s].T
        for i in range(T // sub):
            r = pl.ds(i * sub, sub)
            a, d = A[s, r, :], D[s, r, :]
            for k in range(0, ft, 256):
                k = pl.ds(k, 256)
                gate = dot(a, wbuf[slot, 0, :, k])
                g = sigmoid(gate)
                silu = gate * g
                silus[b, :, k] = silu
                slopes[b, :, k] = g + silu * (1.0 - g)
                dhid = dot_t(d, wbuf[slot, 2, k, :]).astype(BF).astype(F32)
                du[b, r, k] = (dhid * silus[b, :, k]).astype(BF)
                slopes[b, :, k] = slopes[b, :, k] * dhid
                up = dot(a, wbuf[slot, 1, :, k])
                hid[b, r, k] = (silus[b, :, k] * up).astype(BF)
                dg[b, r, k] = (slopes[b, :, k] * up).astype(BF)

    def contract(b):
        ag[...] += dot(AT[b], dg[b])
        au[...] += dot(AT[b], du[b])
        ad[...] += dot(DT[b], hid[b])

    @pl.when(t < n)
    def _():
        for copy in own_factors(t):
            copy.wait()
        AT[0] = A[0].T
        DT[0] = D[0].T
        ag[...] = dot(AT[0], factors[2])
        au[...] = dot(AT[0], factors[1])
        ad[...] = dot(DT[0], factors[0])

    @pl.when(t < n - 1)
    def _():
        for copy in own_factors(t + 1):
            copy.start()

    @pl.when(t >= n)
    def _():
        chain(0, 0)
        ag[...] = dot(AT[0], dg[0])
        au[...] = dot(AT[0], du[0])
        ad[...] = dot(DT[0], hid[0])

    for s in range(1, SIDE):
        chain(s, s % 2)
        if s > 1:
            contract((s - 1) % 2)
        if s == 2:
            pl.when(t >= 1)(functools.partial(total, t - 1))
    contract((SIDE - 1) % 2)

    @pl.when(t == n - 1)
    def _():
        gather.finish()
        for copy in rest:
            copy.wait()
        for copy in second():
            copy.start()

    @pl.when(t == 0)
    def _():
        gather.relay()

    @pl.when(t >= 2)
    def _():
        final(t - 2)

    pack(t)
    for copy in reduction(t)[:4]:
        copy.start()

    @pl.when(t >= 3)
    def _():
        assemble(t - 3)


    @pl.when(t == last)
    def _():
        final(t - 1)
        total(t)
        assemble(t - 2)
        final(t)
        copies = [remote(osq, others.at[k], qsend.at[k], qrecv.at[k], peer) for k, peer in enumerate(peers)]
        for copy in copies:
            copy.start()
        assemble(t - 1)
        assemble(t)
        for copy in copies:
            copy.wait()
        total_squares = osq[...]
        for k in range(len(peers)):
            total_squares += others[k]
        osq[...] = total_squares


def fold(v):
    tiles = [v[i : i + 8, k : k + 128] for i in range(0, v.shape[0], 8) for k in range(0, v.shape[1], 128)]
    while len(tiles) > 1:
        tiles = [a + b for a, b in zip(tiles[::2], tiles[1::2])] + tiles[len(tiles) // 2 * 2 :]
    return tiles[0]


def update_kernel(count, parts, sq, *refs):
    g, m, v, w, nw, nm, nv, bm, bv, bw = (refs[3 * i : 3 * i + 3] for i in range(10))
    came, left = refs[30:]
    mine = lax.axis_index("x") * SIDE + lax.axis_index("y")
    pieces = g[0].shape[0] * parts

    def at(i, k, first=0):
        _, rows, width = g[i].shape
        l, c = lax.div(k, parts), lax.rem(k, parts)
        if i < 2:
            return (l, pl.ds(first, rows), pl.ds(pl.multiple_of(c * (width // parts), width // parts), width // parts))
        return (l, pl.ds(pl.multiple_of(first + c * (rows // parts), rows // parts), rows // parts), slice(None))

    def arrivals(i, k):
        here, there = at(i, k), at(i, k, pl.multiple_of(mine * g[i].shape[1], g[i].shape[1]))
        return [
            pltpu.make_async_copy(m[i].at[here], bm[i].at[here], came.at[i, k, 0]),
            pltpu.make_async_copy(v[i].at[here], bv[i].at[here], came.at[i, k, 1]),
            pltpu.make_async_copy(w[i].at[there], bw[i].at[here], came.at[i, k, 2]),
        ]

    def departures(i, k):
        here = at(i, k)
        return [
            pltpu.make_async_copy(bm[i].at[here], nm[i].at[here], left.at[i, k, 0]),
            pltpu.make_async_copy(bv[i].at[here], nv[i].at[here], left.at[i, k, 1]),
        ]

    def each(do):
        for i in range(3):

            def one(k, _, i=i):
                do(i, k)
                return 0

            lax.fori_loop(0, pieces, one, 0)

    def come(i, k):
        for copy in arrivals(i, k):
            copy.start()

    def work(i, k):
        here = at(i, k)
        for copy in arrivals(i, k):
            copy.wait()
        grad = g[i][here].astype(F32) * factor
        new_m = 0.9 * bm[i][here] + 0.1 * grad
        new_v = 0.95 * bv[i][here] + 0.05 * grad * grad
        wide = bw[i][here].astype(F32)
        step = new_m * lax.rsqrt(new_v + 1e-8) + 0.1 * wide
        nw[i][here] = (wide - 0.02 * step).astype(BF)
        bm[i][here] = new_m
        bv[i][here] = new_v
        for copy in departures(i, k):
            copy.start()

    def leave(i, k):
        for copy in departures(i, k):
            copy.wait()

    each(come)
    factor = jnp.minimum(1.0, 0.5 * lax.rsqrt(jnp.sum(sq[...], keepdims=True) / count + 1e-30))
    each(work)
    each(leave)


def gather_kernel(bg, bu, bd, og, ou, od, local, send, recv):
    x, xa, xb = ring("x")
    y, ya, yb = ring("y")
    greet([{"x": xa}, {"x": xb}, {"y": ya}, {"y": yb}])
    colours = [("x", xa, "y", ya, -1), ("x", xb, "y", yb, 1), ("y", ya, "x", xa, -1), ("y", yb, "x", xb, 1)]
    blocks, outs = (bg, bu, bd), (og, ou, od)

    def owner(colour, i, j):
        first, _, _, _, back = colours[colour]
        i, j = (i, j) if first == "x" else (j, i)
        return lax.rem(x + SIDE + back * i, SIDE) * SIDE + lax.rem(y + SIDE + back * j, SIDE)

    def place(piece, colour, d):
        rows = blocks[piece].shape[1]
        at = pl.multiple_of(d * rows, rows)
        if piece < 2:
            width = bg.shape[2] // 4
            return outs[piece].at[:, pl.ds(at, rows), pl.ds(colour * width, width)]
        return outs[piece].at[:, pl.ds(at + colour * (rows // 4), rows // 4), :]

    def source(piece, colour, i, j):
        if i or j:
            return place(piece, colour, owner(colour, i, j))
        if piece < 2:
            width = bg.shape[2] // 4
            return blocks[piece].at[:, :, pl.ds(colour * width, width)]
        rows = bd.shape[1] // 4
        return bd.at[:, pl.ds(colour * rows, rows), :]

    def hop(piece, colour, i, j, along):
        a, an, b, bn, _ = colours[colour]
        i2, j2 = (i + 1, j) if along == 0 else (i, j + 1)
        return remote(
            source(piece, colour, i, j), place(piece, colour, owner(colour, i, j)),
            send.at[piece, colour, along], recv.at[piece, colour, i2 * SIDE + j2], {a: an} if along == 0 else {b: bn},
        )

    mine = x * SIDE + y
    locals_ = []
    for piece in range(3):
        rows = blocks[piece].shape[1]
        locals_.append(pltpu.make_async_copy(blocks[piece], outs[piece].at[:, pl.ds(pl.multiple_of(mine * rows, rows), rows), :], local.at[piece]))
    events = sorted((12 * p + 3 * i + 4 * j, p, i, j) for p in range(3) for i in range(SIDE) for j in range(SIDE))
    sent = []
    for _, p, i, j in events:
        for c in range(4):
            if i or j:
                hop(p, c, i - 1 if j == 0 else i, j - 1 if j else 0, 0 if j == 0 else 1).wait_recv()
            if j == 0 and i < SIDE - 1:
                copy = hop(p, c, i, j, 0)
                copy.start()
                sent.append(copy)
            if j < SIDE - 1:
                copy = hop(p, c, i, j, 1)
                copy.start()
                sent.append(copy)
        if (p, i, j) == (0, 0, 0):
            for copy in locals_:
                copy.start()
    for copy in sent:
        copy.wait_send()
    for copy in locals_:
        copy.wait()


def out_kernel(src, dst, sem):
    part = src.shape[1] // 4
    copies = []
    for k in range(2 * 4):
        at = (k // 4, pl.ds(k % 4 * part, part))
        copies.append(pltpu.make_async_copy(src.at[at], dst.at[at], sem.at[k]))
    for copy in copies:
        copy.start()
    for copy in copies:
        copy.wait()


def cost(units, w):
    return pl.CostEstimate(flops=units * 2 * 1024 * w.shape[1] * w.shape[2], bytes_accessed=4 * w.size, transcendentals=0)


def params(limit, collective=None):
    if collective is None:
        return pltpu.CompilerParams(vmem_limit_bytes=limit)
    return pltpu.CompilerParams(vmem_limit_bytes=limit, collective_id=collective, has_side_effects=True)


def step(x, dy, wg, wu, wd, mg, mu, md, vg, vu, vd):
    x, dy = x[0], dy[0]
    T, Dm = x.shape
    layers, _, ff = wg.shape
    state = jax.ShapeDtypeStruct((T, Dm), BF)
    slots = jax.ShapeDtypeStruct((3, T, Dm), BF)
    whole = pl.BlockSpec((T, Dm), lambda j: (0, 0))

    tiny = pl.BlockSpec(memory_space=pltpu.VMEM)
    ft = 1024
    steps = ff // ft
    a1, a2, dh1, dys, a2s, a1h, saved = pl.pallas_call(
        functools.partial(chain_kernel, steps),
        grid=(layers * steps,),
        in_specs=[whole, whole] + [ANY] * 4,
        out_specs=[whole] * 3 + [ANY] * 4,
        out_shape=[state] * 3
        + [slots] * 2
        + [jax.ShapeDtypeStruct((2, T // 2, Dm), BF), jax.ShapeDtypeStruct((3, T, ff // SIDE), BF)],
        scratch_shapes=[pltpu.VMEM((T, Dm), BF)]
        + [pltpu.VMEM((T, Dm), F32)] * 2
        + [pltpu.VMEM((2, Dm, ft), BF)] * 2
        + [pltpu.VMEM((2, ft, Dm), BF), pltpu.VMEM((2, 3, T, ft), BF), DMA((2, 3)), DMA((2, 2))]
        + [DMA((6,))] * 4
        + [DMA((2,))] * 2,
        compiler_params=params(60 * MIB, 0),
        cost_estimate=cost(8, wg),
        name="chain",
    )(x, dy, dy, wg, wu, wd)

    ft = 512
    n = ff // (SIDE * ft)
    rows = mg.shape[1]
    piece = 2 * SIDE * rows + ft // SIDE
    vm = pltpu.VMEM
    peers = SIDE * SIDE - 1
    full = lambda *shape: pl.BlockSpec(shape, lambda t: (0,) * len(shape))
    gg, gu, gd, sq, _, _ = pl.pallas_call(
        functools.partial(gradient_kernel, n, rows),
        grid=(layers * n,),
        in_specs=[ANY] * 11,
        out_specs=[tiny] * 4 + [ANY, ANY],
        out_shape=[pltpu.VMEM(m.shape, BF) for m in (mg, mu, md)]
        + [pltpu.VMEM((8, 128), F32), slots, jax.ShapeDtypeStruct((4, T // 2, Dm), BF)],
        scratch_shapes=[vm((SIDE, T, Dm), BF)] * 2
        + [vm((2, Dm, T), BF)] * 2
        + [vm((2, T, ft), BF)] * 3
        + [vm((2, 256, ft), F32)] * 2
        + [vm((Dm, ft), F32)] * 4
        + [vm((2, 3, ft, Dm), BF)]
        + [vm((3, piece, ft), BF)] * 2
        + [vm((3, piece, ft), F32)] * 2
        + [vm((3, piece, ft), BF)] * 4
        + [vm((4, piece, ft), BF), vm((4, 3, 2 * rows, ft), BF), vm((peers, 8, 128), F32), vm((3, T, ft), BF)]
        + [DMA((12,)), DMA((SIDE,)), DMA((2, 12)), DMA((6,)), DMA((6,)), DMA((4,)), DMA((4,)), DMA((3, 6)), DMA((3, 6)), DMA((4, 3)), DMA((4, 3)), DMA((peers,)), DMA((peers,))],
        compiler_params=params(59 * MIB, 1),
        cost_estimate=cost(12, wg),
        name="gradients",
    )(a2, a2s, dy, dys, a1, a1h, dh1, wg, wu, wd, saved)

    count = sum(w.size for w in (wg, wu, wd))
    parts = 4
    shapes = lambda dt: [jax.ShapeDtypeStruct(m.shape, dt) for m in (mg, mu, md)]
    buffers = lambda dt: [vm(m.shape, dt) for m in (mg, mu, md)]
    bg, bu, bd, *moments = pl.pallas_call(
        functools.partial(update_kernel, count, parts),
        in_specs=[tiny] * 4 + [ANY] * 9,
        out_specs=[tiny] * 3 + [ANY] * 6,
        out_shape=buffers(BF) + shapes(F32) + shapes(F32),
        scratch_shapes=buffers(F32) + buffers(F32) + buffers(BF) + [DMA((3, layers * parts, 3)), DMA((3, layers * parts, 2))],
        compiler_params=params(46 * MIB),
        name="update",
    )(sq, gg, gu, gd, mg, mu, md, vg, vu, vd, wg, wu, wd)

    new = pl.pallas_call(
        gather_kernel,
        in_specs=[ANY] * 3,
        out_specs=[tiny] * 3,
        out_shape=[pltpu.VMEM(w.shape, BF) for w in (wg, wu, wd)],
        scratch_shapes=[DMA((3,)), DMA((3, 4, 2)), DMA((3, 4, SIDE * SIDE))],
        compiler_params=params(MIB, 2),
        cost_estimate=cost(24, wg),
        name="gather",
    )(bg, bu, bd)

    new = [
        pl.pallas_call(
            out_kernel,
            in_specs=[tiny],
            out_specs=ANY,
            out_shape=jax.ShapeDtypeStruct(w.shape, BF),
            scratch_shapes=[DMA((8,))],
            compiler_params=params(MIB),
            name="out",
        )(w)
        for w in new
    ]
    return (*new, *moments)


def solution(mesh):
    side = math.isqrt(mesh.shape["dp"])
    torus = Mesh(mesh.devices.reshape(-1, side, side), ("rep", "x", "y"))
    batch = P(("rep", "x", "y"))
    rows = P(None, ("x", "y"))
    out_rows = P("rep", ("x", "y"))
    return jax.shard_map(
        step,
        mesh=torus,
        in_specs=(batch, batch, P(), P(), P(), *[rows] * 6),
        out_specs=(P("rep"),) * 3 + (out_rows,) * 6,
        check_vma=False,
    )
```

```python
import functools
import math

import jax
import jax.numpy as jnp
from jax import lax
from jax.experimental import pallas as pl
from jax.experimental.pallas import tpu as pltpu
from jax.sharding import Mesh
from jax.sharding import PartitionSpec as P

F32, BF = jnp.float32, jnp.bfloat16
MESH = pl.DeviceIdType.MESH
MIB = 2**20
ANY = pl.BlockSpec(memory_space=pl.ANY)
DMA = pltpu.SemaphoreType.DMA
SIDE = 4


def dot(a, b):
    return jnp.dot(a, b, preferred_element_type=F32)


def dot_t(a, b):
    return lax.dot_general(a, b, (((1,), (1,)), ((), ())), preferred_element_type=F32)


def normed(h):
    wide = h.astype(F32)
    scale = lax.rsqrt(jnp.mean(wide * wide, -1, keepdims=True) + 1e-6)
    return (wide * scale).astype(BF)


def sigmoid(z):
    return 0.5 * jnp.tanh(0.5 * z) + 0.5


def ring(axis):
    me = lax.axis_index(axis)
    return me, lax.rem(me + 1, SIDE), lax.rem(me + SIDE - 1, SIDE)


class Place:
    def __init__(self):
        self.turned = lax.rem(lax.axis_index("rep"), 2)
        x, y = lax.axis_index("x"), lax.axis_index("y")
        self.u, self.v = self.pair(x, y)

    def pair(self, a, b):
        return a + self.turned * (b - a), b + self.turned * (a - b)

    def device(self, u, v):
        x, y = self.pair(u, v)
        return {"x": x, "y": y}

    def rank(self, u, v):
        x, y = self.pair(u, v)
        return x * SIDE + y

    def gathering(self, step):
        return self.device(lax.rem(self.u + step, SIDE), self.v)

    def summing(self, step):
        return self.device(self.u, lax.rem(self.v + step, SIDE))


def greet(devices):
    barrier = pltpu.get_barrier_semaphore()
    for device in devices:
        pl.semaphore_signal(barrier, inc=1, device_id=device, device_id_type=MESH)
    pl.semaphore_wait(barrier, len(devices))


def remote(src, dst, send, recv, device):
    return pltpu.make_async_remote_copy(
        src_ref=src, dst_ref=dst, send_sem=send, recv_sem=recv, device_id=device, device_id_type=MESH
    )


class Gather:
    def __init__(self, place, own, slots, send, recv):
        after, before = place.gathering(1), place.gathering(SIDE - 1)
        half = own.shape[0] // 2
        top, bottom = pl.ds(0, half), pl.ds(half, half)
        c = lambda k, src, dst, to: remote(src, dst, send.at[k], recv.at[k], to)
        self.first = [
            c(0, own.at[top], slots.at[0, top], after),
            c(1, own.at[bottom], slots.at[1, bottom], before),
            c(2, own.at[bottom], slots.at[0, bottom], after),
            c(3, own.at[top], slots.at[1, top], before),
        ]
        self.second = [
            c(4, slots.at[0, top], slots.at[2, top], after),
            c(5, slots.at[1, bottom], slots.at[2, bottom], before),
        ]

    def start(self):
        for copy in self.first:
            copy.start()

    def relay(self):
        for copy in self.first[:2]:
            copy.wait_recv()
        for copy in self.second:
            copy.start()

    def finish(self):
        for copy in self.first[2:] + self.second:
            copy.wait_recv()
        for copy in self.first + self.second:
            copy.wait_send()


def chain_kernel(
    steps, x, dy, dy_any, wg_any, wu_any, wd_any, a1, a2, dh1, dys, a2s, halves, saved, h1, accg, accu, bg, bu, bd,
    stage, wsem, ssem, send, recv, send2, recv2, send1, recv1,
):
    j = pl.program_id(0)
    place = Place()
    after, before = place.gathering(1), place.gathering(SIDE - 1)
    half = a1.shape[0] // 2
    gather_dy = Gather(place, dy_any, dys, send, recv)
    gather_a2 = Gather(place, a2, a2s, send2, recv2)
    part = [
        remote(a1.at[pl.ds(0, half)], halves.at[0], send1.at[0], recv1.at[0], after),
        remote(a1.at[pl.ds(half, half)], halves.at[1], send1.at[1], recv1.at[1], before),
    ]
    ft = bg.shape[2]
    tiles = [pl.ds(q, 256) for q in range(0, ft, 256)]

    width = saved.shape[2] // SIDE
    begin = lax.div(place.rank(place.u, 0), ft // width)

    def share(k):
        return lax.rem(k + begin, steps)

    def weights(j):
        layer, slot = lax.div(j, steps), lax.rem(j, 2)
        step = lax.rem(j + layer * begin, steps)
        at = pl.ds(pl.multiple_of(step * ft, ft), ft)
        return [
            pltpu.make_async_copy(wg_any.at[layer, :, at], bg.at[slot], wsem.at[slot, 0]),
            pltpu.make_async_copy(wu_any.at[layer, :, at], bu.at[slot], wsem.at[slot, 1]),
            pltpu.make_async_copy(wd_any.at[layer, at, :], bd.at[slot], wsem.at[slot, 2]),
        ]

    @pl.when(j == 0)
    def _():
        for copy in weights(j):
            copy.start()
        greet([after, before])
        gather_dy.start()
        a1[...] = normed(x[...])
        accg[...] = jnp.zeros_like(accg)

    @pl.when(j == steps // 2)
    def _():
        gather_dy.relay()

    @pl.when(j == steps)
    def _():
        gather_a2.start()
        accg[...] = jnp.zeros_like(accg)
        accu[...] = jnp.zeros_like(accu)

    @pl.when(j == steps + 3)
    def _():
        gather_dy.finish()
        gather_a2.relay()
        for copy in part:
            copy.start()

    k = j - steps

    def kept(k, do):
        for part in range(ft // width):
            block = share(k) * (ft // width) + part
            u, v = place.pair(lax.div(block, SIDE), lax.rem(block, SIDE))
            to = pl.ds(pl.multiple_of(v * width, width), width)

            @pl.when((k >= 0) & (u == place.u))
            def _():
                slot = lax.rem(k, 2)
                do(pltpu.make_async_copy(stage.at[slot, :, :, pl.ds(part * width, width)], saved.at[:, :, to], ssem.at[slot, part]))

    kept(k - 2, lambda copy: copy.wait())

    for copy in weights(j):
        copy.wait()

    @pl.when(j < 2 * steps - 1)
    def _():
        for copy in weights(j + 1):
            copy.start()

    slot = lax.rem(j, 2)
    wg, wu, wd = bg.at[pl.ds(slot, 1)], bu.at[pl.ds(slot, 1)], bd.at[pl.ds(slot, 1)]

    @pl.when(j < steps)
    def _():
        a = a1[...]
        hidden = []
        for q in tiles:
            gate, up = dot(a, wg[0, :, q]), dot(a, wu[0, :, q])
            hidden.append((gate * sigmoid(gate) * up).astype(BF))
        accg[...] += dot(jnp.concatenate(hidden, 1), wd[0])

    @pl.when(j == steps - 1)
    def _():
        h = x[...] + accg[...].astype(BF)
        h1[...] = h
        a2[...] = normed(h)

    @pl.when(j >= steps)
    def _():
        a, d = a2[...], dy[...]
        for q in tiles:
            gate, up = dot(a, wg[0, :, q]), dot(a, wu[0, :, q])
            dhid = dot_t(d, wd[0, q, :]).astype(BF).astype(F32)
            s = sigmoid(gate)
            silu = gate * s
            stage[slot, 0, :, q] = (silu * up).astype(BF)
            stage[slot, 1, :, q] = (dhid * silu).astype(BF)
            stage[slot, 2, :, q] = (dhid * up * (s + silu * (1.0 - s))).astype(BF)
        accu[...] += dot_t(stage[slot, 1], wu[0])
        accg[...] += dot_t(stage[slot, 2], wg[0])

    kept(k, lambda copy: copy.start())

    @pl.when(j == 2 * steps - 1)
    def _():
        da = (accg[...].astype(BF).astype(F32) + accu[...].astype(BF).astype(F32)).astype(BF).astype(F32)
        wide = h1[...].astype(F32)
        scale = lax.rsqrt(jnp.mean(wide * wide, -1, keepdims=True) + 1e-6)
        along = jnp.sum(da * wide, -1, keepdims=True) * (scale * scale * scale * (1.0 / wide.shape[-1]))
        dh1[...] = dy[...] + (da * scale - wide * along).astype(BF)
        for back in (1, 0):
            kept(k - back, lambda copy: copy.wait())
        gather_a2.finish()
        for copy in part:
            copy.wait()


def gate_row(xb, rows):
    return xb * (2 * rows) + lax.div(xb, 2) * (4 * rows)


def gradient_kernel(
    n, rows,
    a2, a2s, dy, dys, a1, a1h, dh1, wg, wu, wd, saved,
    og, ou, od, osq, dslots, b1,
    A, D, AT, DT, hid, dg, du, silus, slopes, ag, au, ad, dT, wbuf, far, raw, keep, own, summed, frecv, rm, rp, GT, XR, others, factors,
    lsem, fsem, wsem, gsend, grecv, bsend, brecv, rsend, rrecv, xsend, xrecv, qsend, qrecv,
):
    t = pl.program_id(0)
    last = 2 * n - 1
    place = Place()
    u, v = place.u, place.v
    after, before = place.gathering(1), place.gathering(SIDE - 1)
    T, Dm = a2.shape
    half = T // 2
    ft = wbuf.shape[2]
    chunk = ft // SIDE
    top, bottom = pl.ds(0, half), pl.ds(half, half)
    gather = Gather(place, dh1, dslots, gsend, grecv)
    bcopy = lambda k, src, to: remote(src, b1.at[k], bsend.at[k], brecv.at[k], to)
    rest = [bcopy(0, a1.at[bottom], after), bcopy(1, a1.at[top], before), bcopy(2, a1h.at[0], after), bcopy(3, a1h.at[1], before)]

    def weights(t):
        layer, j, slot = 1 - lax.div(t, n), lax.rem(t, n), lax.rem(t, 2)
        out = []
        for k in range(SIDE):
            at = pl.multiple_of(place.rank(u, k) * (n * chunk) + j * chunk, chunk)
            to = pl.ds(k * chunk, chunk)
            out.append(pltpu.make_async_copy(wg.at[layer, :, pl.ds(at, chunk)], wbuf.at[slot, 0, :, to], wsem.at[slot, 3 * k]))
            out.append(pltpu.make_async_copy(wu.at[layer, :, pl.ds(at, chunk)], wbuf.at[slot, 1, :, to], wsem.at[slot, 3 * k + 1]))
            out.append(pltpu.make_async_copy(wd.at[layer, pl.ds(at, chunk), :], wbuf.at[slot, 2, to, :], wsem.at[slot, 3 * k + 2]))
        return out

    def loads(pairs):
        return [pltpu.make_async_copy(src, dst, lsem.at[k]) for k, (src, dst) in enumerate(pairs)]

    first = lambda: loads([(a2, A.at[0]), (dy, D.at[0])] + [(a2s.at[k], A.at[k + 1]) for k in range(3)] + [(dys.at[k], D.at[k + 1]) for k in range(3)])
    second = lambda: loads(
        [(a1, A.at[0]), (dh1, D.at[0])]
        + [(a1h.at[0], A.at[1, top]), (b1.at[0], A.at[1, bottom]), (b1.at[1], A.at[2, top]), (a1h.at[1], A.at[2, bottom])]
        + [(b1.at[2], A.at[3, top]), (b1.at[3], A.at[3, bottom])]
        + [(dslots.at[k], D.at[k + 1]) for k in range(3)]
    )

    def own_factors(t):
        out = []
        for k in range(SIDE):
            at = pl.multiple_of(k * (n * chunk) + t * chunk, chunk)
            out.append(pltpu.make_async_copy(saved.at[:, :, pl.ds(at, chunk)], factors.at[:, :, pl.ds(k * chunk, chunk)], fsem.at[k]))
        return out

    def reduction(t):
        s = lax.rem(t, 3)
        h = far.shape[1] // 2
        lo, hi = pl.ds(0, h), pl.ds(h, h)
        next_, last_ = place.summing(1), place.summing(SIDE - 1)
        c = lambda k, src, dst, to: remote(src, dst, rsend.at[s, k], rrecv.at[s, k], to)
        return [
            c(0, far.at[s, lo], frecv.at[s, lo], next_),
            c(1, far.at[s, hi], frecv.at[s, hi], last_),
            c(2, raw.at[s, hi], rm.at[s, hi], next_),
            c(3, raw.at[s, lo], rp.at[s, lo], last_),
            c(4, summed.at[s, lo], rm.at[s, lo], next_),
            c(5, summed.at[s, hi], rp.at[s, hi], last_),
        ]

    def pack(t):
        s = lax.rem(t, 3)
        dT[...] = ad[...].T

        def rows_for(rel):
            vd = lax.rem(v + rel, SIDE)
            parts = {}
            for b in range(SIDE):
                at = pl.multiple_of(place.rank(b, vd) * rows, rows)
                to = b * 2 * rows + (b // 2) * 4 * rows
                parts[to] = ag[pl.ds(at, rows), :]
                parts[to + rows] = au[pl.ds(at, rows), :]
            at = pl.multiple_of(vd * chunk, chunk)
            parts[4 * rows] = dT[pl.ds(at, chunk // 2), :]
            parts[6 * rows] = dT[pl.ds(at + chunk // 2, chunk // 2), :]
            return parts

        h = far.shape[1] // 2
        for to, part in rows_for(2).items():
            far[s, pl.ds(to, part.shape[0]), :] = part.astype(BF)
        for to, part in rows_for(1).items():
            if to < h:
                keep[s, pl.ds(to, part.shape[0]), :] = part
            else:
                raw[s, pl.ds(to, part.shape[0]), :] = part.astype(BF)
        for to, part in rows_for(3).items():
            if to < h:
                raw[s, pl.ds(to, part.shape[0]), :] = part.astype(BF)
            else:
                keep[s, pl.ds(to, part.shape[0]), :] = part
        for to, part in rows_for(0).items():
            own[s, pl.ds(to, part.shape[0]), :] = part

    def total(t):
        s = lax.rem(t, 3)
        copies = reduction(t)
        copies[0].wait_recv()
        copies[1].wait_recv()
        summed[s] = (keep[s] + frecv[s].astype(F32)).astype(BF)
        copies[4].start()
        copies[5].start()

    def across(t):
        out, g = [], lax.rem(t, 4)
        for r in range(1, SIDE):
            to = lax.rem(u + r, SIDE)
            at = pl.multiple_of(gate_row(to, rows), 2 * rows)
            out.append(remote(GT.at[g, pl.ds(at, 2 * rows)], XR.at[g, r - 1], xsend.at[g, r - 1], xrecv.at[g, r - 1], place.device(to, v)))
        return out

    def final(t):
        s, g = lax.rem(t, 3), lax.rem(t, 4)
        copies = reduction(t)
        for copy in copies[2:]:
            copy.wait_recv()
        for copy in copies:
            copy.wait_send()
        mine = (own[s] + rm[s].astype(F32) + rp[s].astype(F32)).astype(BF)
        GT[g] = mine
        for copy in across(t):
            copy.start()
        wide = mine.astype(F32)
        osq[...] += fold(wide * wide)

    def assemble(t):
        layer, j, g = 1 - lax.div(t, n), lax.rem(t, n), lax.rem(t, 4)
        for copy in across(t):
            copy.wait()
        for r in range(SIDE):
            source = lax.rem(u + SIDE - r, SIDE)
            if r:
                piece = XR[g, r - 1]
            else:
                piece = GT[g, pl.ds(pl.multiple_of(gate_row(u, rows), 2 * rows), 2 * rows), :]
            for k in range(SIDE):
                at = pl.multiple_of(place.rank(source, k) * (n * chunk) + j * chunk, chunk)
                og[layer, :, pl.ds(at, chunk)] = piece[:rows, k * chunk : (k + 1) * chunk]
                ou[layer, :, pl.ds(at, chunk)] = piece[rows:, k * chunk : (k + 1) * chunk]
        od[layer, pl.ds(pl.multiple_of(j * chunk, chunk), chunk), :] = GT[g, 4 * rows : 8 * rows, :]

    peers = [place.device(lax.rem(u + i, SIDE), lax.rem(v + k, SIDE)) for i in range(SIDE) for k in range(SIDE)][1:]

    @pl.when(t == 0)
    def _():
        for copy in first() + weights(t) + own_factors(t):
            copy.start()
        greet(peers)
        gather.start()
        for copy in rest:
            copy.start()
        osq[...] = jnp.zeros_like(osq)
        for copy in first()[:2]:
            copy.wait()

    @pl.when(t == n)
    def _():
        for copy in second()[:2]:
            copy.wait()

    for copy in weights(t):
        copy.wait()

    @pl.when(t < last)
    def _():
        for copy in weights(t + 1):
            copy.start()

    slot = lax.rem(t, 2)
    sub = silus.shape[1]
    def chain(s, b):
        AT[b] = A[s].T
        DT[b] = D[s].T
        for i in range(T // sub):
            r = pl.ds(i * sub, sub)
            a, d = A[s, r, :], D[s, r, :]
            for k in range(0, ft, 256):
                k = pl.ds(k, 256)
                gate = dot(a, wbuf[slot, 0, :, k])
                g = sigmoid(gate)
                silu = gate * g
                silus[b, :, k] = silu
                slopes[b, :, k] = g + silu * (1.0 - g)
                dhid = dot_t(d, wbuf[slot, 2, k, :]).astype(BF).astype(F32)
                du[b, r, k] = (dhid * silus[b, :, k]).astype(BF)
                slopes[b, :, k] = slopes[b, :, k] * dhid
                up = dot(a, wbuf[slot, 1, :, k])
                hid[b, r, k] = (silus[b, :, k] * up).astype(BF)
                dg[b, r, k] = (slopes[b, :, k] * up).astype(BF)

    def contract(b):
        ag[...] += dot(AT[b], dg[b])
        au[...] += dot(AT[b], du[b])
        ad[...] += dot(DT[b], hid[b])

    @pl.when(t < n)
    def _():
        for copy in own_factors(t):
            copy.wait()
        AT[0] = A[0].T
        DT[0] = D[0].T
        ag[...] = dot(AT[0], factors[2])
        au[...] = dot(AT[0], factors[1])
        ad[...] = dot(DT[0], factors[0])

    @pl.when(t < n - 1)
    def _():
        for copy in own_factors(t + 1):
            copy.start()

    @pl.when(t >= n)
    def _():
        chain(0, 0)
        ag[...] = dot(AT[0], dg[0])
        au[...] = dot(AT[0], du[0])
        ad[...] = dot(DT[0], hid[0])

    @pl.when(t == 0)
    def _():
        for copy in first()[2:]:
            copy.wait()

    @pl.when(t == n)
    def _():
        for copy in second()[2:]:
            copy.wait()

    for s in range(1, SIDE):
        chain(s, s % 2)
        if s > 1:
            contract((s - 1) % 2)
        if s == 2:
            pl.when(t >= 1)(functools.partial(total, t - 1))
    contract((SIDE - 1) % 2)

    @pl.when(t == n - 1)
    def _():
        gather.finish()
        for copy in rest:
            copy.wait()
        for copy in second():
            copy.start()

    @pl.when(t == 0)
    def _():
        gather.relay()

    @pl.when(t >= 2)
    def _():
        final(t - 2)

    pack(t)
    for copy in reduction(t)[:4]:
        copy.start()

    @pl.when(t >= 3)
    def _():
        assemble(t - 3)


    @pl.when(t == last)
    def _():
        final(t - 1)
        total(t)
        assemble(t - 2)
        final(t)
        copies = [remote(osq, others.at[k], qsend.at[k], qrecv.at[k], peer) for k, peer in enumerate(peers)]
        for copy in copies:
            copy.start()
        assemble(t - 1)
        assemble(t)
        for copy in copies:
            copy.wait()
        total_squares = osq[...]
        for k in range(len(peers)):
            total_squares += others[k]
        osq[...] = total_squares


def fold(v):
    tiles = [v[i : i + 8, k : k + 128] for i in range(0, v.shape[0], 8) for k in range(0, v.shape[1], 128)]
    while len(tiles) > 1:
        tiles = [a + b for a, b in zip(tiles[::2], tiles[1::2])] + tiles[len(tiles) // 2 * 2 :]
    return tiles[0]


def update_kernel(count, parts, sq, *refs):
    g, m, v, w, nw, nm, nv, bm, bv, bw = (refs[3 * i : 3 * i + 3] for i in range(10))
    came, left = refs[30:]
    mine = lax.axis_index("x") * SIDE + lax.axis_index("y")
    pieces = g[0].shape[0] * parts

    def at(i, k, first=0):
        _, rows, width = g[i].shape
        l, c = lax.div(k, parts), lax.rem(k, parts)
        if i < 2:
            return (l, pl.ds(first, rows), pl.ds(pl.multiple_of(c * (width // parts), width // parts), width // parts))
        return (l, pl.ds(pl.multiple_of(first + c * (rows // parts), rows // parts), rows // parts), slice(None))

    def arrivals(i, k):
        here, there = at(i, k), at(i, k, pl.multiple_of(mine * g[i].shape[1], g[i].shape[1]))
        return [
            pltpu.make_async_copy(m[i].at[here], bm[i].at[here], came.at[i, k, 0]),
            pltpu.make_async_copy(v[i].at[here], bv[i].at[here], came.at[i, k, 1]),
            pltpu.make_async_copy(w[i].at[there], bw[i].at[here], came.at[i, k, 2]),
        ]

    def departures(i, k):
        here = at(i, k)
        return [
            pltpu.make_async_copy(bm[i].at[here], nm[i].at[here], left.at[i, k, 0]),
            pltpu.make_async_copy(bv[i].at[here], nv[i].at[here], left.at[i, k, 1]),
        ]

    def each(do):
        for i in range(3):

            def one(k, _, i=i):
                do(i, k)
                return 0

            lax.fori_loop(0, pieces, one, 0)

    def come(i, k):
        for copy in arrivals(i, k):
            copy.start()

    def work(i, k):
        here = at(i, k)
        for copy in arrivals(i, k):
            copy.wait()
        grad = g[i][here].astype(F32) * factor
        new_m = 0.9 * bm[i][here] + 0.1 * grad
        new_v = 0.95 * bv[i][here] + 0.05 * grad * grad
        wide = bw[i][here].astype(F32)
        step = new_m * lax.rsqrt(new_v + 1e-8) + 0.1 * wide
        nw[i][here] = (wide - 0.02 * step).astype(BF)
        bm[i][here] = new_m
        bv[i][here] = new_v
        for copy in departures(i, k):
            copy.start()

    def leave(i, k):
        for copy in departures(i, k):
            copy.wait()

    each(come)
    factor = jnp.minimum(1.0, 0.5 * lax.rsqrt(jnp.sum(sq[...], keepdims=True) / count + 1e-30))
    each(work)
    each(leave)


def gather_kernel(bg, bu, bd, og, ou, od, local, send, recv):
    x, xa, xb = ring("x")
    y, ya, yb = ring("y")
    greet([{"x": xa}, {"x": xb}, {"y": ya}, {"y": yb}])
    colours = [("x", xa, "y", ya, -1), ("x", xb, "y", yb, 1), ("y", ya, "x", xa, -1), ("y", yb, "x", xb, 1)]
    blocks, outs = (bg, bu, bd), (og, ou, od)

    def owner(colour, i, j):
        first, _, _, _, back = colours[colour]
        i, j = (i, j) if first == "x" else (j, i)
        return lax.rem(x + SIDE + back * i, SIDE) * SIDE + lax.rem(y + SIDE + back * j, SIDE)

    def place(piece, colour, d):
        rows = blocks[piece].shape[1]
        at = pl.multiple_of(d * rows, rows)
        if piece < 2:
            width = bg.shape[2] // 4
            return outs[piece].at[:, pl.ds(at, rows), pl.ds(colour * width, width)]
        return outs[piece].at[:, pl.ds(at + colour * (rows // 4), rows // 4), :]

    def source(piece, colour, i, j):
        if i or j:
            return place(piece, colour, owner(colour, i, j))
        if piece < 2:
            width = bg.shape[2] // 4
            return blocks[piece].at[:, :, pl.ds(colour * width, width)]
        rows = bd.shape[1] // 4
        return bd.at[:, pl.ds(colour * rows, rows), :]

    def hop(piece, colour, i, j, along):
        a, an, b, bn, _ = colours[colour]
        i2, j2 = (i + 1, j) if along == 0 else (i, j + 1)
        return remote(
            source(piece, colour, i, j), place(piece, colour, owner(colour, i, j)),
            send.at[piece, colour, along], recv.at[piece, colour, i2 * SIDE + j2], {a: an} if along == 0 else {b: bn},
        )

    mine = x * SIDE + y
    locals_ = []
    for piece in range(3):
        rows = blocks[piece].shape[1]
        locals_.append(pltpu.make_async_copy(blocks[piece], outs[piece].at[:, pl.ds(pl.multiple_of(mine * rows, rows), rows), :], local.at[piece]))
    events = sorted((12 * p + 3 * i + 4 * j, p, i, j) for p in range(3) for i in range(SIDE) for j in range(SIDE))
    sent = []
    for _, p, i, j in events:
        for c in range(4):
            if i or j:
                hop(p, c, i - 1 if j == 0 else i, j - 1 if j else 0, 0 if j == 0 else 1).wait_recv()
            if j == 0 and i < SIDE - 1:
                copy = hop(p, c, i, j, 0)
                copy.start()
                sent.append(copy)
            if j < SIDE - 1:
                copy = hop(p, c, i, j, 1)
                copy.start()
                sent.append(copy)
        if (p, i, j) == (0, 0, 0):
            for copy in locals_:
                copy.start()
    for copy in sent:
        copy.wait_send()
    for copy in locals_:
        copy.wait()


def out_kernel(src, dst, sem):
    part = src.shape[1] // 4
    copies = []
    for k in range(2 * 4):
        at = (k // 4, pl.ds(k % 4 * part, part))
        copies.append(pltpu.make_async_copy(src.at[at], dst.at[at], sem.at[k]))
    for copy in copies:
        copy.start()
    for copy in copies:
        copy.wait()


def cost(units, w):
    return pl.CostEstimate(flops=units * 2 * 1024 * w.shape[1] * w.shape[2], bytes_accessed=4 * w.size, transcendentals=0)


def params(limit, collective=None):
    if collective is None:
        return pltpu.CompilerParams(vmem_limit_bytes=limit)
    return pltpu.CompilerParams(vmem_limit_bytes=limit, collective_id=collective, has_side_effects=True)


def step(x, dy, wg, wu, wd, mg, mu, md, vg, vu, vd):
    x, dy = x[0], dy[0]
    T, Dm = x.shape
    layers, _, ff = wg.shape
    state = jax.ShapeDtypeStruct((T, Dm), BF)
    slots = jax.ShapeDtypeStruct((3, T, Dm), BF)
    whole = pl.BlockSpec((T, Dm), lambda j: (0, 0))

    tiny = pl.BlockSpec(memory_space=pltpu.VMEM)
    ft = 1024
    steps = ff // ft
    a1, a2, dh1, dys, a2s, a1h, saved = pl.pallas_call(
        functools.partial(chain_kernel, steps),
        grid=(layers * steps,),
        in_specs=[whole, whole] + [ANY] * 4,
        out_specs=[whole] * 3 + [ANY] * 4,
        out_shape=[state] * 3
        + [slots] * 2
        + [jax.ShapeDtypeStruct((2, T // 2, Dm), BF), jax.ShapeDtypeStruct((3, T, ff // SIDE), BF)],
        scratch_shapes=[pltpu.VMEM((T, Dm), BF)]
        + [pltpu.VMEM((T, Dm), F32)] * 2
        + [pltpu.VMEM((2, Dm, ft), BF)] * 2
        + [pltpu.VMEM((2, ft, Dm), BF), pltpu.VMEM((2, 3, T, ft), BF), DMA((2, 3)), DMA((2, 2))]
        + [DMA((6,))] * 4
        + [DMA((2,))] * 2,
        compiler_params=params(60 * MIB, 0),
        cost_estimate=cost(8, wg),
        name="chain",
    )(x, dy, dy, wg, wu, wd)

    ft = 512
    n = ff // (SIDE * ft)
    rows = mg.shape[1]
    piece = 2 * SIDE * rows + ft // SIDE
    vm = pltpu.VMEM
    peers = SIDE * SIDE - 1
    full = lambda *shape: pl.BlockSpec(shape, lambda t: (0,) * len(shape))
    gg, gu, gd, sq, _, _ = pl.pallas_call(
        functools.partial(gradient_kernel, n, rows),
        grid=(layers * n,),
        in_specs=[ANY] * 11,
        out_specs=[tiny] * 4 + [ANY, ANY],
        out_shape=[pltpu.VMEM(m.shape, BF) for m in (mg, mu, md)]
        + [pltpu.VMEM((8, 128), F32), slots, jax.ShapeDtypeStruct((4, T // 2, Dm), BF)],
        scratch_shapes=[vm((SIDE, T, Dm), BF)] * 2
        + [vm((2, Dm, T), BF)] * 2
        + [vm((2, T, ft), BF)] * 3
        + [vm((2, 256, ft), F32)] * 2
        + [vm((Dm, ft), F32)] * 4
        + [vm((2, 3, ft, Dm), BF)]
        + [vm((3, piece, ft), BF)] * 2
        + [vm((3, piece, ft), F32)] * 2
        + [vm((3, piece, ft), BF)] * 4
        + [vm((4, piece, ft), BF), vm((4, 3, 2 * rows, ft), BF), vm((peers, 8, 128), F32), vm((3, T, ft), BF)]
        + [DMA((12,)), DMA((SIDE,)), DMA((2, 12)), DMA((6,)), DMA((6,)), DMA((4,)), DMA((4,)), DMA((3, 6)), DMA((3, 6)), DMA((4, 3)), DMA((4, 3)), DMA((peers,)), DMA((peers,))],
        compiler_params=params(59 * MIB, 1),
        cost_estimate=cost(12, wg),
        name="gradients",
    )(a2, a2s, dy, dys, a1, a1h, dh1, wg, wu, wd, saved)

    count = sum(w.size for w in (wg, wu, wd))
    parts = 1
    shapes = lambda dt: [jax.ShapeDtypeStruct(m.shape, dt) for m in (mg, mu, md)]
    buffers = lambda dt: [vm(m.shape, dt) for m in (mg, mu, md)]
    bg, bu, bd, *moments = pl.pallas_call(
        functools.partial(update_kernel, count, parts),
        in_specs=[tiny] * 4 + [ANY] * 9,
        out_specs=[tiny] * 3 + [ANY] * 6,
        out_shape=buffers(BF) + shapes(F32) + shapes(F32),
        scratch_shapes=buffers(F32) + buffers(F32) + buffers(BF) + [DMA((3, layers * parts, 3)), DMA((3, layers * parts, 2))],
        compiler_params=params(46 * MIB),
        name="update",
    )(sq, gg, gu, gd, mg, mu, md, vg, vu, vd, wg, wu, wd)

    new = pl.pallas_call(
        gather_kernel,
        in_specs=[ANY] * 3,
        out_specs=[tiny] * 3,
        out_shape=[pltpu.VMEM(w.shape, BF) for w in (wg, wu, wd)],
        scratch_shapes=[DMA((3,)), DMA((3, 4, 2)), DMA((3, 4, SIDE * SIDE))],
        compiler_params=params(MIB, 2),
        cost_estimate=cost(24, wg),
        name="gather",
    )(bg, bu, bd)

    new = [
        pl.pallas_call(
            out_kernel,
            in_specs=[tiny],
            out_specs=ANY,
            out_shape=jax.ShapeDtypeStruct(w.shape, BF),
            scratch_shapes=[DMA((8,))],
            compiler_params=params(MIB),
            name="out",
        )(w)
        for w in new
    ]
    return (*new, *moments)


def solution(mesh):
    side = math.isqrt(mesh.shape["dp"])
    torus = Mesh(mesh.devices.reshape(-1, side, side), ("rep", "x", "y"))
    batch = P(("rep", "x", "y"))
    rows = P(None, ("x", "y"))
    out_rows = P("rep", ("x", "y"))
    return jax.shard_map(
        step,
        mesh=torus,
        in_specs=(batch, batch, P(), P(), P(), *[rows] * 6),
        out_specs=(P("rep"),) * 3 + (out_rows,) * 6,
        check_vma=False,
    )
```
